32 devices in a mesh: dp: 32 (over z, y, x, core).
Axes of the slice: x: 2, y: 2, z: 4, core: 2. Of those that a mesh axis runs over, the one named last changes fastest.
Arguments:
- local_grads: bfloat16 [32, 32768, 512], P('dp')
- master: float32 [32768, 512], P('dp')
- mom_first: float32 [32768, 512], P('dp')
- mom_second: float32 [32768, 512], P('dp')
- learn_rate: float32 [], replicated
Outputs:
- output 1: float32 [32768, 512], P('dp')
- output 2: float32 [32768, 512], P('dp')
- output 3: float32 [32768, 512], P('dp')
- output 4: bfloat16 [32768, 512], replicated
All inputs are finite; a program needn't handle non-finite values.
Results may differ from the reference program's by a relative error of at most 0.001.
Values are sent between devices in bfloat16 or wider.
A program may use at most 1 GiB of HBM per device.

```python
import math
import jax
import jax.numpy as jnp
import numpy as np
from jax import lax

D = 512
ROWS_DEV = 1024
DEVICES = 32
LAYERS = 2
MIX_RANK = 32
DECAY_RANK = 64
ADAM_STEP = 10


def rule_table(model_width, total_rows):
    ffn_width = 7 * model_width // 2
    layer_rows = 6 * model_width + 2 * ffn_width + 16 + 10 * MIX_RANK + 2 * DECAY_RANK
    vocab_rows = (total_rows - LAYERS * layer_rows - 4) // 2
    base_rule = (1.0, 0.0)
    decay_rule = (1.0, 0.1)
    time_rule = (2.0, 0.0)
    pieces = [(vocab_rows, decay_rule)]
    for layer_idx in range(LAYERS):
        lead_rows = 12 if layer_idx == 0 else 10
        pieces = pieces + [(lead_rows + 10 * MIX_RANK, base_rule), (1, time_rule), (2 * DECAY_RANK, base_rule), (1, time_rule), (5 * model_width, decay_rule), (4, base_rule), (2 * ffn_width + model_width, decay_rule)]
    pieces = pieces + [(2, base_rule), (vocab_rows, decay_rule)]
    run_lengths = np.array([run_len for run_len, run_rule in pieces])
    lr_factor = np.repeat(np.array([run_rule[0] for run_len, run_rule in pieces]), run_lengths)
    decay_rate = np.repeat(np.array([run_rule[1] for run_len, run_rule in pieces]), run_lengths)
    return lr_factor, decay_rate


def setup_inputs(seed: int = 0) -> dict:
    key_grad, key_master, key_first, key_second, key_rate = jax.random.split(jax.random.key(seed), 5)
    total_rows = DEVICES * ROWS_DEV
    elem_count = total_rows * D
    grad_scale = 3.0 * math.sqrt(DEVICES / elem_count)
    clip_unit = 1.0 / math.sqrt(elem_count)

    def draw_device(dev_key):
        gauss_noise = jax.random.normal(dev_key, (total_rows, D), jnp.float32)
        return (grad_scale * gauss_noise).astype(jnp.bfloat16)

    local_grads = lax.map(draw_device, jax.random.split(key_grad, DEVICES))
    master = (0.5 / math.sqrt(D)) * jax.random.normal(key_master, (total_rows, D), jnp.float32)
    mom_first = 0.1 * clip_unit * jax.random.normal(key_first, (total_rows, D), jnp.float32)
    mom_second = jnp.square(0.1 * clip_unit * jax.random.uniform(key_second, (total_rows, D), jnp.float32, 0.5, 1.5))
    learn_rate = jax.random.uniform(key_rate, (), jnp.float32, 0.005, 0.015)
    return {'local_grads': local_grads, 'master': master, 'mom_first': mom_first, 'mom_second': mom_second, 'learn_rate': learn_rate}


def reference(local_grads, master, mom_first, mom_second, learn_rate):
    def add_device(running, grad_block):
        return running + grad_block.astype(jnp.float32), None

    grad_total = lax.scan(add_device, jnp.zeros(master.shape, jnp.float32), local_grads)[0]
    grad_mean = grad_total / local_grads.shape[0]
    grad_norm = jnp.sqrt(jnp.sum(grad_mean * grad_mean))
    clip_scale = jnp.minimum(1.0, 1.0 / (grad_norm + 1e-6))
    clipped = grad_mean * clip_scale
    new_first = 0.9 * mom_first + 0.1 * clipped
    new_second = 0.99 * mom_second + 0.01 * (clipped * clipped)
    first_hat = new_first / (1.0 - 0.9 ** ADAM_STEP)
    second_hat = new_second / (1.0 - 0.99 ** ADAM_STEP)
    lr_factor, decay_rate = rule_table(master.shape[1], master.shape[0])
    row_rate = learn_rate * jnp.asarray(lr_factor, jnp.float32)[:, None]
    row_decay = jnp.asarray(decay_rate, jnp.float32)[:, None]
    new_master = master - row_rate * (first_hat / (jnp.sqrt(second_hat) + 1e-8) + row_decay * master)
    return new_master, new_first, new_second, new_master.astype(jnp.bfloat16)
```

```python
import functools
import jax
import jax.numpy as jnp
from jax import lax
from jax.experimental import pallas as pl
from jax.experimental.pallas import tpu as pltpu
from jax.sharding import PartitionSpec as P

LAYERS = 2
MIX_RANK = 32
DECAY_RANK = 64
ADAM_STEP = 10
STREAMS = 4
MESH = pl.DeviceIdType.MESH

END_JOBS = [
    ("first", 2, 0), ("first", 2, 1), ("first", 3, 1), ("first", 1, 1),
    ("up", 2, 0), ("up", 2, 1), ("pre", 3, 1),
    ("first", 3, 0), ("first", 1, 0), ("first", 0, 1), ("first", 0, 0),
    ("up", 1, 1), ("up", 3, 0), ("up", 1, 0), ("fin", 0, 1), ("res", 0, 0),
]
MID_JOBS = [
    ("first", 3, 1), ("first", 2, 0), ("first", 0, 1), ("first", 2, 1),
    ("up", 3, 1),
    ("first", 3, 0), ("first", 1, 1), ("first", 0, 0), ("first", 1, 0),
    ("up", 2, 0), ("down", 0, 1), ("up", 2, 1), ("fin", 1, 1), ("up", 3, 0), ("down", 0, 0), ("res", 1, 0),
]
END_EVENTS = [(0, 1, "u"), (1, 0, ""), (2, 0, ""), (3, 0, "q"), (1, 1, ""), (3, 1, ""), (2, 1, "")]
MID_EVENTS = [(2, 0, "d"), (0, 0, "u"), (1, 1, "u"), (0, 1, "u"), (3, 0, "de"), (2, 1, "d"), (3, 1, "")]


def rule_runs(model_width, total_rows):
    ffn_width = 7 * model_width // 2
    layer_rows = 6 * model_width + 2 * ffn_width + 16 + 10 * MIX_RANK + 2 * DECAY_RANK
    vocab_rows = (total_rows - LAYERS * layer_rows - 4) // 2
    decay_runs = [(0, vocab_rows)]
    fast_rows = []
    row = vocab_rows
    for layer_idx in range(LAYERS):
        row = row + (12 if layer_idx == 0 else 10) + 10 * MIX_RANK
        fast_rows.append(row)
        row = row + 1 + 2 * DECAY_RANK
        fast_rows.append(row)
        row = row + 1
        decay_runs.append((row, row + 5 * model_width))
        row = row + 5 * model_width + 4
        decay_runs.append((row, row + 2 * ffn_width + model_width))
        row = row + 2 * ffn_width + model_width
    row = row + 2
    decay_runs.append((row, row + vocab_rows))
    return decay_runs, fast_rows


def step_kernel(
    lr_ref, grads, master, mom1, mom2,
    o_master, o_mom1, o_mom2, o_work, praw,
    stg, acc, zd, zu, pre, fin, rb, wbuf, nsum, nb, nr,
    core_s, core_r, first_s, first_r, z_s, zd_r, zu_r, q_s, pre_r, fin_r,
    ld, st_ld, st_out, own_out, norm_s, norm_r,
    gat_r, gcore_r, gcore_s, gp_s, gup_s, gdn_s, gq_s,
):
    rows, width = acc.shape[2], acc.shape[3]
    shard = STREAMS * rows
    total_rows = grads.shape[1]
    tile = min(32, rows)
    me = lax.axis_index("dp")
    c, x, y, z = me % 2, (me // 2) % 2, (me // 4) % 2, me // 8
    lo = 1 - z // 2
    m = lo * z + (1 - lo) * (3 - z)
    sgn = 2 * lo - 1

    def dev(zz, yy, xx, cc):
        return ((zz * 2 + yy) * 2 + xx) * 2 + cc

    partner = dev(z, y, x, 1 - c)
    xn, yn = dev(z, y, 1 - x, c), dev(z, 1 - y, x, c)
    up = dev(z + sgn, y, x, c)
    down = dev(z - sgn, y, x, c)
    zothers = [dev((z + d) % 4, y, x, c) for d in (1, 2, 3)]

    def pn(s):
        h = s % 2
        return xn * (1 - h) + yn * h

    def qn(s):
        h = s % 2
        return yn * (1 - h) + xn * h

    def chip(s, u, qo, po):
        h = s % 2
        first = x * (1 - h) + y * h
        last = y * (1 - h) + x * h
        pv = 1 - first if po else first
        qv = 1 - last if qo else last
        xx = pv * (1 - h) + qv * h
        yy = qv * (1 - h) + pv * h
        return ((lo * u + (1 - lo) * (3 - u)) * 2 + yy) * 2 + xx

    def remote(src, dst, ssem, rsem, to):
        return pltpu.make_async_remote_copy(
            src_ref=src, dst_ref=dst, send_sem=ssem, recv_sem=rsem, device_id=(to,), device_id_type=MESH
        )

    def each(n, body):
        def step(i, carry):
            body(i)
            return carry

        lax.fori_loop(0, n, step, 0)

    barrier = pltpu.get_barrier_semaphore()
    for other in [partner, xn, yn] + zothers:
        pl.semaphore_signal(barrier, inc=1, device_id=(other,), device_id_type=MESH)
    pl.semaphore_wait(barrier, 6)

    def grad_rows(ci, s, cc):
        return grads.at[0, pl.ds(pl.multiple_of((ci * 2 + cc) * shard + s * rows, rows), rows)]

    def praw_rows(ci, s):
        return praw.at[pl.ds(pl.multiple_of((ci * STREAMS + s) * rows, rows), rows)]

    def core_copy(ci, s):
        i = ci * STREAMS + s
        return remote(grad_rows(ci, s, 1 - c), praw_rows(ci, s), core_s.at[i], core_r.at[i], partner)

    def loads(job, slot, s):
        ci = chip(s, job[1], job[2], job[0] == "first")
        own = pltpu.make_async_copy(grad_rows(ci, s, c), rb.at[slot, s, 0], ld.at[slot, s, 0])
        other = pltpu.make_async_copy(praw_rows(ci, s), rb.at[slot, s, 1], ld.at[slot, s, 1])
        return ci, own, other

    def prefetch(job, slot):
        def body(s):
            ci, own, other = loads(job, slot, s)
            core_copy(ci, s).wait_recv()
            own.start()
            other.start()

        each(STREAMS, body)

    def landed(ref, rsem):
        remote(ref, ref, z_s.at[0, 0], rsem, me).wait_recv()

    def sent(ref, ssem):
        remote(ref, ref, ssem, zu_r.at[0, 0], me).wait_send()

    def run_job(job, slot, mid, zslot):
        kind, u, qo = job
        k = 2 * u + qo

        def body(s):
            _, own, other = loads(job, slot, s)
            parts = []
            if kind != "first":
                parts.append((acc.at[s, k], first_r.at[s, k]))
                from_down = mid and u >= 1 and not (u == 3 and qo == 1)
                from_up = (mid and u <= 1) or (not mid and u == 0)
                if from_down:
                    parts.append((zd.at[s, k - 2], zd_r.at[s, k - 2]))
                if from_up:
                    parts.append((zu.at[s, k], zu_r.at[s, k]))
                if not mid and (u, qo) == (3, 0):
                    parts.append((pre.at[s], pre_r.at[s]))
                if kind == "res":
                    parts.append((fin.at[s], fin_r.at[s]))
            for ref, rsem in parts:
                landed(ref, rsem)
            own.wait()
            other.wait()
            dst = stg.at[s, k] if kind == "first" else acc.at[s, k]

            def add(t):
                at = pl.ds(pl.multiple_of(t * tile, tile), tile)
                v = rb[slot, s, 0, at, :].astype(jnp.float32) + rb[slot, s, 1, at, :].astype(jnp.float32)
                for ref, _ in parts:
                    v = v + ref[at, :]
                if kind == "res":
                    v = v * (1.0 / 32.0)
                    nsum[...] += jnp.sum((v * v).reshape(tile // 8, 8, width), axis=0)
                dst[at, :] = v

            each(rows // tile, add)
            if kind == "first":
                remote(dst, acc.at[s, k], first_s.at[s, k], first_r.at[s, k], pn(s)).start()
            elif kind == "pre":
                remote(dst, pre.at[s], q_s.at[s, 0], pre_r.at[s], qn(s)).start()
            elif kind == "fin":
                remote(dst, fin.at[s], q_s.at[s, 1], fin_r.at[s], qn(s)).start()
            elif kind == "up" and not mid:
                remote(dst, zd.at[s, k - 2], z_s.at[s, zslot], zd_r.at[s, k - 2], up).start()
            elif kind == "up":
                kk = 2 * (3 - u) + qo
                remote(dst, zu.at[s, kk], z_s.at[s, zslot], zu_r.at[s, kk], up).start()
            elif kind == "down":
                remote(dst, zu.at[s, k], z_s.at[s, zslot], zu_r.at[s, k], down).start()

        each(STREAMS, body)

    def state_load(s):
        at = pl.ds(pl.multiple_of(s * rows, rows), rows)
        return [
            pltpu.make_async_copy(ref.at[at], stg.at[i, s], st_ld.at[i, s])
            for i, ref in enumerate((master, mom1, mom2))
        ]

    def state_store(s):
        at = pl.ds(pl.multiple_of(s * rows, rows), rows)
        return [
            pltpu.make_async_copy(stg.at[i, s], ref.at[at], st_out.at[i, s])
            for i, ref in enumerate((o_master, o_mom1, o_mom2))
        ]

    def reduce_program(jobs, mid):
        order = [j for j in jobs if j[0] == "first"] + [j for j in jobs if j[0] != "first"]
        for kind, u, qo in order:
            each(STREAMS, lambda s: core_copy(chip(s, u, qo, kind == "first"), s).start())
        prefetch(jobs[0], 0)
        zslot = 0
        for j, job in enumerate(jobs):
            if j + 1 < len(jobs):
                prefetch(jobs[j + 1], (j + 1) % 2)
            if job[0] == "res":
                each(8 * STREAMS, lambda i: sent(stg.at[i // 8, i % 8], first_s.at[i // 8, i % 8]))

                def start_state(s):
                    for copy in state_load(s):
                        copy.start()

                each(STREAMS, start_state)
            run_job(job, j % 2, mid, zslot)
            if job[0] in ("up", "down"):
                zslot += 1
        each(zslot * STREAMS, lambda i: sent(acc.at[0, 0], z_s.at[i // zslot, i % zslot]))
        if not mid:
            each(STREAMS, lambda s: sent(acc.at[0, 0], q_s.at[s, 0]))
        each(STREAMS, lambda s: sent(acc.at[0, 0], q_s.at[s, 1]))

    nsum[...] = jnp.zeros_like(nsum)

    @pl.when(m == 0)
    def _():
        reduce_program(END_JOBS, False)

    @pl.when(m == 1)
    def _():
        reduce_program(MID_JOBS, True)

    part = nsum[:, 0:128]
    for col in range(128, width, 128):
        part = part + nsum[:, col:col + 128]
    for i, other in enumerate((partner, xn, yn)):
        nb[i] = part
        copy = remote(nb.at[i], nr.at[i], norm_s.at[i], norm_r.at[i], other)
        copy.start()
        copy.wait()
        part = part + nr[i]
    nb[3] = part
    for i, other in enumerate(zothers):
        remote(nb.at[3], nr.at[3 + i], norm_s.at[3 + i], norm_r.at[3 + i], other).start()
    for i in range(3):
        sent(nb.at[3], norm_s.at[3 + i])
        landed(nr.at[3 + i], norm_r.at[3 + i])
    square_sum = jnp.sum((part + nr[4]) + (nr[3] + nr[5]), keepdims=True)
    clip = jnp.minimum(1.0, 1.0 / (jnp.sqrt(square_sum) + 1e-6))
    clip = jnp.broadcast_to(clip, (tile, 128))

    learn_rate = lr_ref[0]
    inv1 = 1.0 / (1.0 - 0.9 ** ADAM_STEP)
    inv2 = 1.0 / (1.0 - 0.99 ** ADAM_STEP)
    decay_runs, fast_rows = rule_runs(width, total_rows)
    my_chip = me // 2

    def work_rows(ci, s, cc):
        return o_work.at[pl.ds(pl.multiple_of((ci * 2 + cc) * shard + s * rows, rows), rows)]

    def own_store(s):
        return pltpu.make_async_copy(wbuf.at[s], work_rows(my_chip, s, c), own_out.at[s])

    def pass_on(src, ci, s, ssem, to):
        remote(src, work_rows(ci, s, c), ssem, gat_r.at[ci * STREAMS + s], to).start()

    def to_core(src, ci, s):
        i = ci * STREAMS + s
        remote(src, work_rows(ci, s, c), gcore_s.at[i], gcore_r.at[i], partner).start()

    def update(s):
        for copy in state_load(s):
            copy.wait()

        def rows_step(t):
            base = pl.multiple_of(t * tile, tile)
            at = pl.ds(base, tile)
            row = me * shard + s * rows + base + lax.broadcasted_iota(jnp.int32, (tile, 128), 0)
            decays = (row >= decay_runs[0][0]) & (row < decay_runs[0][1])
            for start, stop in decay_runs[1:]:
                decays = decays | ((row >= start) & (row < stop))
            fast = row == fast_rows[0]
            for fast_row in fast_rows[1:]:
                fast = fast | (row == fast_row)
            decay = jnp.where(decays, 0.1, 0.0)
            step_size = learn_rate * jnp.where(fast, 2.0, 1.0)
            for col in range(0, width, 128):
                cols = pl.ds(col, 128)
                g = acc[s, 2 * m, at, cols] * clip
                old = stg[0, s, at, cols]
                first = 0.9 * stg[1, s, at, cols] + 0.1 * g
                second = 0.99 * stg[2, s, at, cols] + 0.01 * (g * g)
                new = old - step_size * ((first * inv1) / (jnp.sqrt(second * inv2) + 1e-8) + decay * old)
                stg[0, s, at, cols] = new
                stg[1, s, at, cols] = first
                stg[2, s, at, cols] = second
                wbuf[s, at, cols] = new.astype(jnp.bfloat16)

        each(rows // tile, rows_step)
        pass_on(wbuf.at[s], my_chip, s, gq_s.at[s, 0], qn(s))
        pass_on(wbuf.at[s], my_chip, s, gup_s.at[s, 0], up)

        @pl.when(m == 1)
        def _():
            pass_on(wbuf.at[s], my_chip, s, gdn_s.at[s, 0], down)

        pass_on(wbuf.at[s], my_chip, s, gp_s.at[s, 0], pn(s))
        to_core(wbuf.at[s], my_chip, s)
        own_store(s).start()
        for copy in state_store(s):
            copy.start()

    each(STREAMS, update)

    def arrive(s, u, qo, po):
        ci = chip(s, u, qo, po)
        ref = work_rows(ci, s, c)
        landed(ref, gat_r.at[ci * STREAMS + s])
        return ci, ref

    def gather_program(events, own):
        passed = [(own, 0)]
        ups, downs = 1, 1
        for n, (u, qo, links) in enumerate(events):
            def event(s, ups=ups, downs=downs):
                ci, ref = arrive(s, u, qo, 0)
                if "u" in links:
                    pass_on(ref, ci, s, gup_s.at[s, ups], up)
                if "d" in links:
                    pass_on(ref, ci, s, gdn_s.at[s, downs], down)
                if "e" in links:
                    ce = chip(s, 1, 1, 0)
                    pass_on(work_rows(ce, s, c), ce, s, gdn_s.at[s, downs + 1], down)
                if "q" in links:
                    pass_on(ref, ci, s, gq_s.at[s, 1], qn(s))
                pass_on(ref, ci, s, gp_s.at[s, n + 1], pn(s))
                to_core(ref, ci, s)

            each(STREAMS, event)
            ups += links.count("u")
            downs += links.count("d") + links.count("e")
            passed.append((u, qo))
            if n >= 1:
                other_side(*passed[n - 1])
        for u, qo in passed[len(events) - 1:]:
            other_side(u, qo)
        mid = own == 1
        block = wbuf.at[0]
        each(ups * STREAMS, lambda i: sent(block, gup_s.at[i // ups, i % ups]))
        if mid:
            each(downs * STREAMS, lambda i: sent(block, gdn_s.at[i // downs, i % downs]))
        else:
            each(STREAMS, lambda s: sent(block, gq_s.at[s, 1]))

    def other_side(u, qo):
        def body(s):
            ci, ref = arrive(s, u, qo, 1)
            to_core(ref, ci, s)

        each(STREAMS, body)

    @pl.when(m == 0)
    def _():
        gather_program(END_EVENTS, 0)

    @pl.when(m == 1)
    def _():
        gather_program(MID_EVENTS, 1)

    block = wbuf.at[0]

    def drain(s):
        sent(block, gq_s.at[s, 0])
        own_store(s).wait()
        for copy in state_store(s):
            copy.wait()

    each(STREAMS, drain)
    each(8 * STREAMS, lambda i: sent(block, gp_s.at[i // 8, i % 8]))

    def drain_core(i):
        ci, s = i // STREAMS, i % STREAMS
        core_copy(ci, s).wait_send()
        sent(block, gcore_s.at[i])
        landed(work_rows(ci, s, 1 - c), gcore_r.at[i])

    each(16 * STREAMS, drain_core)


def solution(mesh):
    dev_count = mesh.shape["dp"]

    def device_step(local_grads, master, mom_first, mom_second, learn_rate):
        shard_rows, width = master.shape
        total_rows = shard_rows * dev_count
        rows = shard_rows // STREAMS
        any_spec = pl.BlockSpec(memory_space=pl.ANY)
        dma = pltpu.SemaphoreType.DMA
        f32, bf16 = jnp.float32, jnp.bfloat16
        shard = jax.ShapeDtypeStruct((shard_rows, width), f32)
        outs = pl.pallas_call(
            step_kernel,
            out_shape=[
                shard, shard, shard,
                jax.ShapeDtypeStruct((total_rows, width), bf16),
                jax.ShapeDtypeStruct((total_rows // 2, width), bf16),
            ],
            in_specs=[pl.BlockSpec(memory_space=pltpu.SMEM)] + [any_spec] * 4,
            out_specs=[any_spec] * 5,
            scratch_shapes=[
                pltpu.VMEM((STREAMS, 8, rows, width), f32),
                pltpu.VMEM((STREAMS, 8, rows, width), f32),
                pltpu.VMEM((STREAMS, 5, rows, width), f32),
                pltpu.VMEM((STREAMS, 4, rows, width), f32),
                pltpu.VMEM((STREAMS, rows, width), f32),
                pltpu.VMEM((STREAMS, rows, width), f32),
                pltpu.VMEM((2, STREAMS, 2, rows, width), bf16),
                pltpu.VMEM((STREAMS, rows, width), bf16),
                pltpu.VMEM((8, width), f32),
                pltpu.VMEM((4, 8, 128), f32),
                pltpu.VMEM((6, 8, 128), f32),
                dma((16 * STREAMS,)), dma((16 * STREAMS,)),
                dma((STREAMS, 8)), dma((STREAMS, 8)),
                dma((STREAMS, 6)), dma((STREAMS, 5)), dma((STREAMS, 4)),
                dma((STREAMS, 2)), dma((STREAMS,)), dma((STREAMS,)),
                dma((2, STREAMS, 2)), dma((3, STREAMS)), dma((3, STREAMS)), dma((STREAMS,)),
                dma((6,)), dma((6,)),
                dma((16 * STREAMS,)), dma((16 * STREAMS,)), dma((16 * STREAMS,)),
                dma((STREAMS, 8)), dma((STREAMS, 4)), dma((STREAMS, 5)), dma((STREAMS, 2)),
            ],
            compiler_params=pltpu.CompilerParams(
                collective_id=0, has_side_effects=True, vmem_limit_bytes=67043328
            ),
            name="adam_step",
        )(learn_rate.reshape(1), local_grads, master, mom_first, mom_second)
        return outs[0], outs[1], outs[2], outs[3]

    return jax.shard_map(
        device_step,
        mesh=mesh,
        in_specs=(P("dp", None, None), P("dp", None), P("dp", None), P("dp", None), P()),
        out_specs=(P("dp", None), P("dp", None), P("dp", None), P(None, None)),
        check_vma=False,
    )
```

```python
import jax
import jax.numpy as jnp
from jax import lax
from jax.experimental import pallas as pl
from jax.experimental.pallas import tpu as pltpu
from jax.sharding import PartitionSpec as P

LAYERS = 2
MIX_RANK = 32
DECAY_RANK = 64
ADAM_STEP = 10
STREAMS = 8
GROUP = 4
MESH = pl.DeviceIdType.MESH

END_JOBS = [
    ("first", 2, 0, 1), ("first", 2, 1, 1), ("first", 2, 0, 0), ("first", 3, 1, 1), ("up", 2, 0, 1),
    ("up", 2, 1, 1), ("first", 1, 1, 1), ("first", 1, 0, 0), ("up", 1, 1, 1), ("first", 2, 1, 0),
    ("first", 3, 1, 0), ("up", 2, 1, 0), ("pre", 3, 1, 0), ("first", 1, 1, 0), ("first", 3, 0, 0),
    ("up", 2, 0, 0), ("up", 1, 1, 0), ("pre", 3, 1, 1), ("first", 0, 1, 0), ("first", 3, 0, 1),
    ("first", 0, 1, 1), ("up", 3, 0, 0), ("up", 3, 0, 1), ("first", 1, 0, 1), ("fin", 0, 1, 1),
    ("fin", 0, 1, 0), ("up", 1, 0, 0), ("first", 0, 0, 0), ("first", 0, 0, 1), ("up", 1, 0, 1),
    ("res", 0, 0, 0), ("res", 0, 0, 1),
]
MID_JOBS = [
    ("first", 3, 1, 0), ("first", 3, 1, 1), ("first", 2, 0, 1), ("first", 1, 0, 1), ("up", 2, 0, 1),
    ("up", 3, 1, 1), ("first", 2, 1, 0), ("first", 2, 1, 1), ("first", 0, 1, 0), ("first", 1, 1, 0),
    ("first", 3, 0, 1), ("first", 0, 1, 1), ("up", 3, 1, 0), ("first", 3, 0, 0), ("up", 2, 1, 0),
    ("first", 1, 1, 1), ("up", 2, 1, 1), ("first", 0, 0, 0), ("first", 0, 0, 1), ("down", 0, 1, 0),
    ("first", 2, 0, 0), ("down", 0, 1, 1), ("up", 3, 0, 0), ("down", 0, 0, 0), ("up", 3, 0, 1),
    ("fin", 1, 1, 0), ("first", 1, 0, 0), ("fin", 1, 1, 1), ("down", 0, 0, 1), ("up", 2, 0, 0),
    ("res", 1, 0, 0), ("res", 1, 0, 1),
]
END_SENDS = [
    (0, 0, 0, "q", 0), (0, 0, 0, "q", 1), (0, 0, 0, "u", 0), (0, 0, 0, "u", 1), (0, 0, 0, "p", 0),
    (0, 0, 0, "p", 1), (0, 0, 0, "c", 0), (0, 0, 0, "c", 1), (1, 0, 0, "p", 1), (0, 1, 0, "u", 0),
    (0, 0, 1, "c", 1), (0, 1, 0, "u", 1), (0, 1, 0, "p", 1), (1, 0, 0, "p", 0), (3, 0, 0, "p", 0),
    (1, 0, 0, "c", 1), (3, 0, 0, "c", 0), (0, 1, 0, "p", 0), (3, 0, 0, "q", 0), (3, 0, 0, "q", 1),
    (2, 0, 0, "c", 0), (3, 1, 0, "c", 0), (2, 0, 0, "p", 0), (3, 0, 0, "c", 1), (0, 1, 0, "c", 1),
    (0, 1, 1, "c", 0), (3, 0, 0, "p", 1), (2, 0, 0, "p", 1), (0, 1, 0, "c", 0), (3, 1, 0, "p", 0),
    (3, 0, 1, "c", 0), (2, 1, 0, "p", 0), (2, 0, 1, "c", 1), (3, 0, 1, "c", 1), (2, 0, 0, "c", 1),
    (3, 1, 0, "c", 1), (1, 1, 0, "p", 1), (3, 1, 0, "p", 1), (0, 0, 1, "c", 0), (2, 1, 0, "p", 1),
    (1, 1, 0, "c", 1), (2, 1, 0, "c", 0), (1, 1, 1, "c", 1), (0, 1, 1, "c", 1), (1, 0, 1, "c", 1),
    (2, 0, 1, "c", 0), (2, 1, 0, "c", 1), (3, 1, 1, "c", 1), (2, 1, 1, "c", 0), (3, 1, 1, "c", 0),
    (1, 0, 0, "c", 0), (1, 1, 0, "p", 0), (2, 1, 1, "c", 1), (1, 1, 0, "c", 0), (1, 0, 1, "c", 0),
    (1, 1, 1, "c", 0),
]
MID_SENDS = [
    (1, 0, 0, "q", 0), (1, 0, 0, "q", 1), (1, 0, 0, "u", 0), (1, 0, 0, "u", 1), (1, 0, 0, "d", 0),
    (1, 0, 0, "d", 1), (1, 0, 0, "p", 0), (1, 0, 0, "p", 1), (1, 0, 0, "c", 0), (1, 0, 0, "c", 1),
    (2, 0, 0, "d", 0), (0, 0, 0, "u", 0), (0, 0, 0, "p", 1), (2, 0, 0, "c", 1), (2, 0, 0, "p", 1),
    (2, 0, 0, "p", 0), (0, 0, 0, "u", 1), (3, 0, 0, "d", 0), (1, 1, 0, "u", 0), (0, 1, 0, "p", 0),
    (1, 1, 0, "u", 1), (1, 1, 0, "p", 1), (3, 0, 0, "p", 0), (3, 0, 0, "d", 1), (0, 1, 0, "p", 1),
    (2, 0, 0, "c", 0), (2, 0, 0, "d", 1), (1, 1, 0, "d", 1), (0, 1, 0, "u", 1), (2, 1, 0, "d", 0),
    (0, 1, 0, "c", 0), (0, 1, 0, "u", 0), (0, 0, 0, "p", 0), (2, 0, 1, "c", 0), (3, 0, 1, "c", 0),
    (2, 1, 0, "p", 1), (1, 1, 0, "p", 0), (0, 0, 0, "c", 0), (2, 1, 0, "d", 1), (2, 1, 1, "c", 1),
    (1, 1, 0, "c", 0), (2, 0, 1, "c", 1), (2, 1, 0, "p", 0), (3, 1, 0, "p", 1), (1, 1, 1, "c", 0),
    (3, 0, 0, "c", 1), (0, 1, 1, "c", 1), (1, 1, 0, "c", 1), (2, 1, 0, "c", 1), (0, 1, 1, "c", 0),
    (1, 1, 0, "d", 0), (3, 1, 0, "c", 1), (0, 0, 1, "c", 1), (3, 1, 0, "p", 0), (3, 0, 0, "p", 1),
    (0, 0, 0, "c", 1), (0, 0, 1, "c", 0), (2, 1, 0, "c", 0), (1, 1, 1, "c", 1), (3, 1, 1, "c", 1),
    (1, 0, 1, "c", 1), (0, 1, 0, "c", 1), (2, 1, 1, "c", 0), (3, 0, 0, "c", 0), (1, 0, 1, "c", 0),
    (3, 1, 0, "c", 0), (3, 1, 1, "c", 0), (3, 0, 1, "c", 1),
]


def rule_runs(model_width, total_rows):
    ffn_width = 7 * model_width // 2
    layer_rows = 6 * model_width + 2 * ffn_width + 16 + 10 * MIX_RANK + 2 * DECAY_RANK
    vocab_rows = (total_rows - LAYERS * layer_rows - 4) // 2
    decay_runs = [(0, vocab_rows)]
    fast_rows = []
    row = vocab_rows
    for layer_idx in range(LAYERS):
        row = row + (12 if layer_idx == 0 else 10) + 10 * MIX_RANK
        fast_rows.append(row)
        row = row + 1 + 2 * DECAY_RANK
        fast_rows.append(row)
        row = row + 1
        decay_runs.append((row, row + 5 * model_width))
        row = row + 5 * model_width + 4
        decay_runs.append((row, row + 2 * ffn_width + model_width))
        row = row + 2 * ffn_width + model_width
    row = row + 2
    decay_runs.append((row, row + vocab_rows))
    return decay_runs, fast_rows


def each(start, stop, body):
    def step(i, carry):
        body(i)
        return carry

    lax.fori_loop(start, stop, step, 0)


def remote(src, dst, ssem, rsem, to):
    return pltpu.make_async_remote_copy(
        src_ref=src, dst_ref=dst, send_sem=ssem, recv_sem=rsem, device_id=(to,), device_id_type=MESH
    )


class Place:
    def __init__(self):
        self.me = me = lax.axis_index("dp")
        self.c, self.x, self.y, self.z = c, x, y, z = me % 2, (me // 2) % 2, (me // 4) % 2, me // 8
        self.lo = 1 - z // 2
        self.m = self.lo * z + (1 - self.lo) * (3 - z)
        sgn = 2 * self.lo - 1
        self.partner = self.dev(z, y, x, 1 - c)
        self.xn, self.yn = self.dev(z, y, 1 - x, c), self.dev(z, 1 - y, x, c)
        self.up = self.dev(z + sgn, y, x, c)
        self.down = self.dev(z - sgn, y, x, c)
        self.flat = me % 8
        self.zothers = [((z + d) % 4) * 8 + self.flat for d in (1, 2, 3)]
        self.plane = [z * 8 + (self.flat + d) % 8 for d in range(1, 8)]

    def dev(self, zz, yy, xx, cc):
        return ((zz * 2 + yy) * 2 + xx) * 2 + cc

    def pn(self, s):
        h = s % 2
        return self.xn * (1 - h) + self.yn * h

    def qn(self, s):
        h = s % 2
        return self.yn * (1 - h) + self.xn * h

    def chip(self, s, u, qo, po):
        h = s % 2
        first = self.x * (1 - h) + self.y * h
        last = self.y * (1 - h) + self.x * h
        pv = 1 - first if po else first
        qv = 1 - last if qo else last
        xx = pv * (1 - h) + qv * h
        yy = qv * (1 - h) + pv * h
        return ((self.lo * u + (1 - self.lo) * (3 - u)) * 2 + yy) * 2 + xx


def enter(others):
    barrier = pltpu.get_barrier_semaphore()
    for other in others:
        pl.semaphore_signal(barrier, inc=1, device_id=(other,), device_id_type=MESH)
    pl.semaphore_wait(barrier, len(others))


def reduce_kernel(
    lr_ref, grads, master, mom1, mom2,
    o_master, o_mom1, o_mom2, o_work, praw,
    stg, acc, zd, zu, fin, rb, nsum, nb, nr, nz,
    core_s, core_r, first_s, first_r, z_s, zd_r, zu_r, q_s, pre_r, fin_r, ld, st_ld, norm_s, norm_r,
):
    rows, width = acc.shape[2], acc.shape[3]
    shard = STREAMS * rows
    total_rows = grads.shape[1]
    tile = min(32, rows)
    at_dev = Place()
    me, c, m, chip, pn, qn = at_dev.me, at_dev.c, at_dev.m, at_dev.chip, at_dev.pn, at_dev.qn

    enter(at_dev.plane + at_dev.zothers)

    def grad_rows(ci, s, cc):
        return grads.at[0, pl.ds(pl.multiple_of((ci * 2 + cc) * shard + s * rows, rows), rows)]

    def praw_rows(ci, s):
        return praw.at[pl.ds(pl.multiple_of((ci * STREAMS + s) * rows, rows), rows)]

    def core_copy(ci, s):
        i = ci * STREAMS + s
        return remote(grad_rows(ci, s, 1 - c), praw_rows(ci, s), core_s.at[i], core_r.at[i], at_dev.partner)

    def each_of(group, body):
        each(group * GROUP, group * GROUP + GROUP, body)

    def loads(job, slot, s):
        kind, u, qo, group = job
        ci = chip(s, u, qo, kind == "first")
        i = s - group * GROUP
        own = pltpu.make_async_copy(grad_rows(ci, s, c), rb.at[slot, i, 0], ld.at[slot, i, 0])
        other = pltpu.make_async_copy(praw_rows(ci, s), rb.at[slot, i, 1], ld.at[slot, i, 1])
        return ci, own, other

    def swap(job):
        kind, u, qo, group = job
        each_of(group, lambda s: core_copy(chip(s, u, qo, kind == "first"), s).start())

    def prefetch(job, slot):
        def body(s):
            ci, own, other = loads(job, slot, s)
            core_copy(ci, s).wait_recv()
            own.start()
            other.start()

        each_of(job[3], body)

    def landed(ref, rsem):
        remote(ref, ref, core_s.at[0], rsem, me).wait_recv()

    def sent(ref, ssem):
        remote(ref, ref, ssem, core_r.at[0], me).wait_send()

    def run_job(job, slot, mid):
        kind, u, qo, group = job
        k = 2 * u + qo

        def body(s):
            _, own, other = loads(job, slot, s)
            parts = []
            if kind != "first":
                parts.append((acc.at[s, k], first_r.at[s, k]))
                if mid and u >= 1 and not (u == 3 and qo == 1):
                    parts.append((zd.at[s, k - 2], zd_r.at[s, k - 2]))
                if (mid and u <= 1) or (not mid and u == 0):
                    parts.append((zu.at[s, k], zu_r.at[s, k]))
                if not mid and (u, qo) == (3, 0):
                    parts.append((zd.at[s, 0], pre_r.at[s]))
                if kind == "res":
                    parts.append((fin.at[s], fin_r.at[s]))
            for ref, rsem in parts:
                landed(ref, rsem)
            own.wait()
            other.wait()
            dst = stg.at[s, k] if kind == "first" else acc.at[s, k]
            i = s - group * GROUP

            def add(t):
                at = pl.ds(pl.multiple_of(t * tile, tile), tile)
                v = rb[slot, i, 0, at, :].astype(jnp.float32) + rb[slot, i, 1, at, :].astype(jnp.float32)
                for ref, _ in parts:
                    v = v + ref[at, :]
                if kind == "res":
                    v = v * (1.0 / 32.0)
                    nsum[...] += jnp.sum((v * v).reshape(tile // 8, 8, width), axis=0)
                dst[at, :] = v

            each(0, rows // tile, add)
            if kind == "first":
                remote(dst, acc.at[s, k], first_s.at[s, k], first_r.at[s, k], pn(s)).start()
            elif kind == "pre":
                remote(dst, zd.at[s, 0], q_s.at[s, 0], pre_r.at[s], qn(s)).start()
            elif kind == "fin":
                remote(dst, fin.at[s], q_s.at[s, 1], fin_r.at[s], qn(s)).start()
            elif kind == "up" and not mid:
                remote(dst, zd.at[s, k - 2], z_s.at[s, k], zd_r.at[s, k - 2], at_dev.up).start()
            elif kind == "up":
                kk = 2 * (3 - u) + qo
                remote(dst, zu.at[s, kk], z_s.at[s, k], zu_r.at[s, kk], at_dev.up).start()
            elif kind == "down":
                remote(dst, zu.at[s, k], z_s.at[s, k], zu_r.at[s, k], at_dev.down).start()

        each_of(group, body)

    def state_load(s):
        at = pl.ds(pl.multiple_of(s * rows, rows), rows)
        return [
            pltpu.make_async_copy(src.at[at], dst.at[at], st_ld.at[i, s])
            for i, (src, dst) in enumerate(((master, o_master), (mom1, o_mom1), (mom2, o_mom2)))
        ]

    def start_state(s):
        for copy in state_load(s):
            copy.start()

    def reduce_program(jobs, mid):
        ahead = 3
        for job in jobs[:ahead]:
            swap(job)
        prefetch(jobs[0], 0)
        for j, job in enumerate(jobs):
            if j + ahead < len(jobs):
                swap(jobs[j + ahead])
            if j + 1 < len(jobs):
                prefetch(jobs[j + 1], (j + 1) % 2)
            run_job(job, j % 2, mid)
            if j == 16:
                each(0, STREAMS, start_state)

    nsum[...] = jnp.zeros_like(nsum)

    @pl.when(m == 0)
    def _():
        reduce_program(END_JOBS, False)

    @pl.when(m == 1)
    def _():
        reduce_program(MID_JOBS, True)

    def all_sum(part, place, count, others, slots, src, base):
        src[...] = part
        slots[place] = part
        for i, (other, _) in enumerate(others):
            remote(src, slots.at[place], norm_s.at[base + i], norm_r.at[base + place], other).start()
        for i, (_, slot) in enumerate(others):
            landed(slots.at[slot], norm_r.at[base + slot])
        total = slots[0]
        for i in range(1, count):
            total = total + slots[i]
        return total

    part = nsum[:, 0:128]
    for col in range(128, width, 128):
        part = part + nsum[:, col:col + 128]
    flat, z = at_dev.flat, at_dev.z
    part = all_sum(part, flat, 8, [(d, (flat + i + 1) % 8) for i, d in enumerate(at_dev.plane)], nr, nb.at[0], 0)
    part = all_sum(part, z, 4, [(d, (z + i + 1) % 4) for i, d in enumerate(at_dev.zothers)], nz, nb.at[1], 8)
    square_sum = jnp.sum(part, keepdims=True)
    clip = jnp.minimum(1.0, 1.0 / (jnp.sqrt(square_sum) + 1e-6))
    clip = jnp.broadcast_to(clip, (tile, 128))

    learn_rate = lr_ref[0]
    inv1 = 1.0 / (1.0 - 0.9 ** ADAM_STEP)
    inv2 = 1.0 / (1.0 - 0.99 ** ADAM_STEP)
    decay_runs, fast_rows = rule_runs(width, total_rows)

    def update(s):
        for copy in state_load(s):
            copy.wait()

        def rows_step(t):
            base = pl.multiple_of(t * tile, tile)
            at = pl.ds(base, tile)
            out_at = pl.ds(pl.multiple_of(s * rows + t * tile, tile), tile)
            row = me * shard + s * rows + base + lax.broadcasted_iota(jnp.int32, (tile, 128), 0)
            decays = (row >= decay_runs[0][0]) & (row < decay_runs[0][1])
            for start, stop in decay_runs[1:]:
                decays = decays | ((row >= start) & (row < stop))
            fast = row == fast_rows[0]
            for fast_row in fast_rows[1:]:
                fast = fast | (row == fast_row)
            decay = jnp.where(decays, 0.1, 0.0)
            step_size = learn_rate * jnp.where(fast, 2.0, 1.0)
            for col in range(0, width, 128):
                cols = pl.ds(col, 128)
                g = acc[s, 2 * m, at, cols] * clip
                old = o_master[out_at, cols]
                first = 0.9 * o_mom1[out_at, cols] + 0.1 * g
                second = 0.99 * o_mom2[out_at, cols] + 0.01 * (g * g)
                new = old - step_size * ((first * inv1) / (jnp.sqrt(second * inv2) + 1e-8) + decay * old)
                o_master[out_at, cols] = new
                o_mom1[out_at, cols] = first
                o_mom2[out_at, cols] = second
                o_work[out_at, cols] = new.astype(jnp.bfloat16)

        each(0, rows // tile, rows_step)

    each(0, STREAMS, update)

    block = acc.at[0, 0]

    def drain(jobs):
        for kind, u, qo, group in jobs:
            k = 2 * u + qo
            if kind == "first":
                each_of(group, lambda s: sent(block, first_s.at[s, k]))
            elif kind in ("up", "down"):
                each_of(group, lambda s: sent(block, z_s.at[s, k]))

    @pl.when(m == 0)
    def _():
        drain([j for j in END_JOBS if j[0] != "first"])
        each(0, STREAMS, lambda s: sent(block, q_s.at[s, 0]))

    @pl.when(m == 1)
    def _():
        drain([j for j in MID_JOBS if j[0] != "first"])

    each(0, 8 * STREAMS, lambda i: sent(block, first_s.at[i // 8, i % 8]))
    each(0, STREAMS, lambda s: sent(block, q_s.at[s, 1]))
    each(0, 16 * STREAMS, lambda i: core_copy(i // STREAMS, i % STREAMS).wait_send())
    for i in range(7):
        sent(nb.at[0], norm_s.at[i])
    for i in range(3):
        sent(nb.at[1], norm_s.at[8 + i])


def gather_kernel(own_ref, o_work, own_s, gat_r, gcore_r, gcore_s, gp_s, gu_s, gd_s, gq_s):
    shard, width = own_ref.shape
    rows = shard // STREAMS
    at_dev = Place()
    me, c, m, chip = at_dev.me, at_dev.c, at_dev.m, at_dev.chip
    my_chip = me // 2

    enter([at_dev.partner, at_dev.xn, at_dev.yn] + at_dev.zothers)

    def work_rows(ci, s, cc):
        return o_work.at[pl.ds(pl.multiple_of((ci * 2 + cc) * shard + s * rows, rows), rows)]

    def send(src, ci, s, k, link):
        dst = work_rows(ci, s, c)
        i = ci * STREAMS + s
        if link == "c":
            remote(src, dst, gcore_s.at[i], gcore_r.at[i], at_dev.partner).start()
        else:
            to = {"p": at_dev.pn(s), "q": at_dev.qn(s), "u": at_dev.up, "d": at_dev.down}[link]
            ssem = {"p": gp_s, "q": gq_s, "u": gu_s, "d": gd_s}[link]
            remote(src, dst, ssem.at[s, k], gat_r.at[i], to).start()

    def gather_program(sends, own):
        first = [t for t in sends if t[:3] == own and t[4] == 0]

        def start_own(s):
            src = own_ref.at[pl.ds(pl.multiple_of(s * rows, rows), rows)]
            for u, qo, _, link, _ in first:
                send(src, my_chip, s, 2 * u + qo, link)

        each(0, STREAMS, start_own)

        def keep(t):
            at = pl.multiple_of(t * 32, 32)
            o_work[pl.ds(pl.multiple_of(me * shard + at, 32), 32), :] = own_ref[pl.ds(at, 32), :]

        each(0, shard // 32, keep)
        rest = [t for t in sends if t[:3] != own]
        seen = set()
        n = 0
        while n < len(rest):
            block, group = rest[n][:3], rest[n][4]
            links = [rest[n][3]]
            while n + 1 < len(rest) and rest[n + 1][:3] == block and rest[n + 1][4] == group:
                n += 1
                links.append(rest[n][3])
            n += 1
            new = (block, group) not in seen
            seen.add((block, group))

            def body(s, block=block, links=tuple(links), new=new):
                ci = chip(s, *block)
                ref = work_rows(ci, s, c)
                if new:
                    remote(ref, ref, gcore_s.at[0], gat_r.at[ci * STREAMS + s], me).wait_recv()
                for link in links:
                    send(ref, ci, s, 2 * block[0] + block[1], link)

            each(group * GROUP, group * GROUP + GROUP, body)
        block_ref = own_ref.at[pl.ds(0, rows)]
        for link, ssem in (("p", gp_s), ("q", gq_s), ("u", gu_s), ("d", gd_s)):
            for k in sorted({2 * t[0] + t[1] for t in sends if t[3] == link}):
                each(0, STREAMS, lambda s: remote(block_ref, block_ref, ssem.at[s, k], gat_r.at[0], me).wait_send())

    @pl.when(m == 0)
    def _():
        gather_program(END_SENDS, (0, 0, 0))

    @pl.when(m == 1)
    def _():
        gather_program(MID_SENDS, (1, 0, 0))

    def drain_core(i):
        ci, s = i // STREAMS, i % STREAMS
        ref = work_rows(ci, s, 1 - c)
        remote(ref, ref, gcore_s.at[i], gcore_r.at[i], me).wait()

    each(0, 16 * STREAMS, drain_core)


def store_kernel(*refs):
    ins, outs, sem = refs[:4], refs[4:8], refs[8]
    copies = [pltpu.make_async_copy(src, dst, sem.at[i]) for i, (src, dst) in enumerate(zip(ins[:3], outs[:3]))]
    pieces = sem.shape[0] - 3
    rows = ins[3].shape[0] // pieces
    for i in range(pieces):
        at = pl.ds(i * rows, rows)
        copies.append(pltpu.make_async_copy(ins[3].at[at], outs[3].at[at], sem.at[3 + i]))
    for copy in copies:
        copy.start()
    for copy in copies:
        copy.wait()


def solution(mesh):
    dev_count = mesh.shape["dp"]

    def device_step(local_grads, master, mom_first, mom_second, learn_rate):
        shard_rows, width = master.shape
        total_rows = shard_rows * dev_count
        rows = shard_rows // STREAMS
        any_spec = pl.BlockSpec(memory_space=pl.ANY)
        vmem_spec = pl.BlockSpec(memory_space=pltpu.VMEM)
        dma = pltpu.SemaphoreType.DMA
        f32, bf16 = jnp.float32, jnp.bfloat16
        shard = pltpu.VMEM((shard_rows, width), f32)
        new_master, new_first, new_second, own_rows, _ = pl.pallas_call(
            reduce_kernel,
            out_shape=[
                shard, shard, shard,
                pltpu.VMEM((shard_rows, width), bf16),
                jax.ShapeDtypeStruct((total_rows // 2, width), bf16),
            ],
            in_specs=[pl.BlockSpec(memory_space=pltpu.SMEM)] + [any_spec] * 4,
            out_specs=[vmem_spec] * 4 + [any_spec],
            scratch_shapes=[
                pltpu.VMEM((STREAMS, 8, rows, width), f32),
                pltpu.VMEM((STREAMS, 8, rows, width), f32),
                pltpu.VMEM((STREAMS, 5, rows, width), f32),
                pltpu.VMEM((STREAMS, 4, rows, width), f32),
                pltpu.VMEM((STREAMS, rows, width), f32),
                pltpu.VMEM((2, GROUP, 2, rows, width), bf16),
                pltpu.VMEM((8, width), f32),
                pltpu.VMEM((2, 8, 128), f32),
                pltpu.VMEM((8, 8, 128), f32),
                pltpu.VMEM((4, 8, 128), f32),
                dma((16 * STREAMS,)), dma((16 * STREAMS,)),
                dma((STREAMS, 8)), dma((STREAMS, 8)),
                dma((STREAMS, 8)), dma((STREAMS, 5)), dma((STREAMS, 4)),
                dma((STREAMS, 2)), dma((STREAMS,)), dma((STREAMS,)),
                dma((2, GROUP, 2)), dma((3, STREAMS)),
                dma((12,)), dma((12,)),
            ],
            compiler_params=pltpu.CompilerParams(
                collective_id=0, has_side_effects=True, vmem_limit_bytes=56 * 2 ** 20
            ),
            name="reduce_update",
        )(learn_rate.reshape(1), local_grads, master, mom_first, mom_second)
        working = pl.pallas_call(
            gather_kernel,
            out_shape=pltpu.VMEM((total_rows, width), bf16),
            in_specs=[vmem_spec],
            out_specs=vmem_spec,
            scratch_shapes=[
                dma((STREAMS,)), dma((16 * STREAMS,)), dma((16 * STREAMS,)), dma((16 * STREAMS,)),
                dma((STREAMS, 8)), dma((STREAMS, 8)), dma((STREAMS, 8)), dma((STREAMS, 8)),
            ],
            compiler_params=pltpu.CompilerParams(
                collective_id=1, has_side_effects=True, vmem_limit_bytes=4 * 2 ** 20
            ),
            name="gather_rows",
        )(own_rows)
        return pl.pallas_call(
            store_kernel,
            out_shape=[jax.ShapeDtypeStruct((shard_rows, width), f32)] * 3
            + [jax.ShapeDtypeStruct((total_rows, width), bf16)],
            in_specs=[vmem_spec] * 4,
            out_specs=[any_spec] * 4,
            scratch_shapes=[dma((3 + 8,))],
            compiler_params=pltpu.CompilerParams(vmem_limit_bytes=4 * 2 ** 20),
            name="store",
        )(new_master, new_first, new_second, working)

    return jax.shard_map(
        device_step,
        mesh=mesh,
        in_specs=(P("dp", None, None), P("dp", None), P("dp", None), P("dp", None), P()),
        out_specs=(P("dp", None), P("dp", None), P("dp", None), P(None, None)),
        check_vma=False,
    )
```

```python
import jax
import jax.numpy as jnp
from jax import lax
from jax.experimental import pallas as pl
from jax.experimental.pallas import tpu as pltpu
from jax.sharding import PartitionSpec as P

LAYERS = 2
MIX_RANK = 32
DECAY_RANK = 64
ADAM_STEP = 10
STREAMS = 16
GROUP = 8
LAG = 20
MESH = pl.DeviceIdType.MESH


def decode(codes):
    return [tuple(int(ch) if ch.isdigit() else ch for ch in code) for code in codes]


END_JOBS = decode([
    "f210", "f201", "u210", "f211", "f200", "f301", "u211", "f110", "u200", "f310", "u110", "u201",
    "f300", "f311", "p310", "f011", "f100", "f111", "u300", "p311", "f101", "u111", "u301", "n011",
    "u100", "f010", "f000", "n010", "f001", "u101", "r000", "r001",
])
MID_JOBS = decode([
    "f211", "f311", "f310", "u311", "f010", "f011", "u310", "f300", "d011", "f200", "f210", "f101",
    "f201", "u200", "u211", "d010", "f301", "f100", "u210", "f111", "f110", "f000", "f001", "u300",
    "n110", "u201", "d000", "n111", "u301", "d001", "r100", "r101",
])
END_SENDS = decode([
    "000q0", "000q1", "000u0", "000u1", "000p0", "000p1", "000c0", "000c1", "100p0", "100c1", "010u1", "010p0",
    "200p1", "010c0", "010p1", "300p0", "300q0", "010u0", "310p0", "100p1", "201c1", "300p1", "300q1", "200p0",
    "011c0", "001c1", "310p1", "300c1", "310c1", "100c0", "210p1", "210c1", "301c0", "301c1", "300c0", "110p1",
    "101c1", "200c0", "200c1", "110c1", "101c0", "201c0", "001c0", "010c1", "110p0", "211c1", "110c0", "311c0",
    "311c1", "111c1", "111c0", "310c0", "210p0", "210c0", "011c1", "211c0",
])
MID_SENDS = decode([
    "100q0", "100q1", "100u0", "100u1", "100d0", "100d1", "100p0", "100p1", "100c0", "100c1", "200p0", "000p0",
    "200d1", "000p1", "000u0", "000u1", "110u1", "101c0", "200c0", "300d0", "200d0", "200p1", "010c1", "110p1",
    "110c1", "300p0", "300d1", "110d1", "300p1", "111c1", "201c1", "110u0", "010u0", "210d1", "110p0", "301c1",
    "010c0", "000c1", "201c0", "001c0", "010u1", "210p1", "300c0", "210c0", "010p1", "010p0", "310c0", "110d0",
    "111c0", "310p0", "210c1", "210p0", "300c1", "310p1", "301c0", "200c1", "101c1", "011c1", "311c0", "211c1",
    "011c0", "210d0", "310c1", "000c0", "311c1", "211c0", "110c0", "001c1",
])


def rule_runs(model_width, total_rows):
    ffn_width = 7 * model_width // 2
    layer_rows = 6 * model_width + 2 * ffn_width + 16 + 10 * MIX_RANK + 2 * DECAY_RANK
    vocab_rows = (total_rows - LAYERS * layer_rows - 4) // 2
    decay_runs = [(0, vocab_rows)]
    fast_rows = []
    row = vocab_rows
    for layer_idx in range(LAYERS):
        row = row + (12 if layer_idx == 0 else 10) + 10 * MIX_RANK
        fast_rows.append(row)
        row = row + 1 + 2 * DECAY_RANK
        fast_rows.append(row)
        row = row + 1
        decay_runs.append((row, row + 5 * model_width))
        row = row + 5 * model_width + 4
        decay_runs.append((row, row + 2 * ffn_width + model_width))
        row = row + 2 * ffn_width + model_width
    row = row + 2
    decay_runs.append((row, row + vocab_rows))
    return decay_runs, fast_rows


def each(start, stop, body):
    def step(i, carry):
        body(i)
        return carry

    lax.fori_loop(start, stop, step, 0)


def remote(src, dst, ssem, rsem, to):
    return pltpu.make_async_remote_copy(
        src_ref=src, dst_ref=dst, send_sem=ssem, recv_sem=rsem, device_id=(to,), device_id_type=MESH
    )


class Place:
    def __init__(self):
        self.me = me = lax.axis_index("dp")
        self.c, self.x, self.y, self.z = c, x, y, z = me % 2, (me // 2) % 2, (me // 4) % 2, me // 8
        self.lo = 1 - z // 2
        self.m = self.lo * z + (1 - self.lo) * (3 - z)
        sgn = 2 * self.lo - 1
        self.partner = self.dev(z, y, x, 1 - c)
        self.xn, self.yn = self.dev(z, y, 1 - x, c), self.dev(z, 1 - y, x, c)
        self.up = self.dev(z + sgn, y, x, c)
        self.down = self.dev(z - sgn, y, x, c)
        self.flat = me % 8
        self.zothers = [((z + d) % 4) * 8 + self.flat for d in (1, 2, 3)]
        self.plane = [z * 8 + (self.flat + d) % 8 for d in range(1, 8)]

    def dev(self, zz, yy, xx, cc):
        return ((zz * 2 + yy) * 2 + xx) * 2 + cc

    def pn(self, s):
        h = s % 2
        return self.xn * (1 - h) + self.yn * h

    def qn(self, s):
        h = s % 2
        return self.yn * (1 - h) + self.xn * h

    def chip(self, s, u, qo, po):
        h = s % 2
        first = self.x * (1 - h) + self.y * h
        last = self.y * (1 - h) + self.x * h
        pv = 1 - first if po else first
        qv = 1 - last if qo else last
        xx = pv * (1 - h) + qv * h
        yy = qv * (1 - h) + pv * h
        return ((self.lo * u + (1 - self.lo) * (3 - u)) * 2 + yy) * 2 + xx


def enter(others):
    barrier = pltpu.get_barrier_semaphore()
    for other in others:
        pl.semaphore_signal(barrier, inc=1, device_id=(other,), device_id_type=MESH)
    pl.semaphore_wait(barrier, len(others))


def reduce_kernel(
    lr_ref, grads, master, mom1, mom2,
    o_master, o_mom1, o_mom2, o_work, praw,
    stg, acc, zd, zu, fin, rb, nsum, nb, nr, nz,
    core_s, core_r, first_s, first_r, z_s, zd_r, zu_r, q_s, pre_r, fin_r, ld, st_ld, norm_s, norm_r,
):
    rows, width = acc.shape[2], acc.shape[3]
    shard = STREAMS * rows
    total_rows = grads.shape[1]
    tile = min(32, rows)
    at_dev = Place()
    me, c, m, chip, pn, qn = at_dev.me, at_dev.c, at_dev.m, at_dev.chip, at_dev.pn, at_dev.qn

    enter(at_dev.plane + at_dev.zothers)

    def grad_rows(ci, s, cc):
        return grads.at[0, pl.ds(pl.multiple_of((ci * 2 + cc) * shard + s * rows, rows), rows)]

    def praw_rows(ci, s):
        return praw.at[pl.ds(pl.multiple_of((ci * STREAMS + s) * rows, rows), rows)]

    def core_copy(ci, s, dst=None):
        i = ci * STREAMS + s
        dst = praw_rows(ci, s) if dst is None else dst
        return remote(grad_rows(ci, s, 1 - c), dst, core_s.at[i], core_r.at[i], at_dev.partner)

    def each_of(group, body):
        each(group * GROUP, group * GROUP + GROUP, body)

    def loads(job, j, s):
        kind, u, qo, group = job
        ci = chip(s, u, qo, kind == "f")
        slot, i = j % 2, s - group * GROUP
        own = pltpu.make_async_copy(grad_rows(ci, s, c), rb.at[slot, i, 0], ld.at[slot, i, 0])
        if j < 2:
            return own, core_copy(ci, s, rb.at[slot, i, 1]), None
        return own, core_copy(ci, s), pltpu.make_async_copy(praw_rows(ci, s), rb.at[slot, i, 1], ld.at[slot, i, 1])

    def swap(job, j):
        each_of(job[3], lambda s: loads(job, j, s)[1].start())

    def prefetch(job, j):
        def body(s):
            own, core, other = loads(job, j, s)
            own.start()
            if other is not None:
                core.wait_recv()
                other.start()

        each_of(job[3], body)

    def landed(ref, rsem):
        remote(ref, ref, core_s.at[0], rsem, me).wait_recv()

    def sent(ref, ssem):
        remote(ref, ref, ssem, core_r.at[0], me).wait_send()

    def run_job(job, j, mid):
        kind, u, qo, group = job
        k = 2 * u + qo
        slot = j % 2

        def body(s):
            own, core, other = loads(job, j, s)
            parts = []
            if kind != "f":
                parts.append((acc.at[s, k], first_r.at[s, k]))
                if mid and u >= 1 and not (u == 3 and qo == 1):
                    parts.append((zd.at[s, k - 2], zd_r.at[s, k - 2]))
                if (mid and u <= 1) or (not mid and u == 0):
                    parts.append((zu.at[s, k], zu_r.at[s, k]))
                if not mid and (u, qo) == (3, 0):
                    parts.append((zd.at[s, 0], pre_r.at[s]))
                if kind == "r":
                    parts.append((fin.at[s], fin_r.at[s]))
            for ref, rsem in parts:
                landed(ref, rsem)
            own.wait()
            if other is None:
                core.wait_recv()
            else:
                other.wait()
            dst = stg.at[s, k] if kind == "f" else acc.at[s, k]
            i = s - group * GROUP

            def add(t):
                at = pl.ds(pl.multiple_of(t * tile, tile), tile)
                v = rb[slot, i, 0, at, :].astype(jnp.float32) + rb[slot, i, 1, at, :].astype(jnp.float32)
                for ref, _ in parts:
                    v = v + ref[at, :]
                if kind == "r":
                    v = v * (1.0 / 32.0)
                    nsum[...] += jnp.sum((v * v).reshape(tile // 8, 8, width), axis=0)
                dst[at, :] = v

            each(0, rows // tile, add)
            if kind == "f":
                remote(dst, acc.at[s, k], first_s.at[s, k], first_r.at[s, k], pn(s)).start()
            elif kind == "p":
                remote(dst, zd.at[s, 0], q_s.at[s, 0], pre_r.at[s], qn(s)).start()
            elif kind == "n":
                remote(dst, fin.at[s], q_s.at[s, 1], fin_r.at[s], qn(s)).start()
            elif kind == "u" and not mid:
                remote(dst, zd.at[s, k - 2], z_s.at[s, k], zd_r.at[s, k - 2], at_dev.up).start()
            elif kind == "u":
                kk = 2 * (3 - u) + qo
                remote(dst, zu.at[s, kk], z_s.at[s, k], zu_r.at[s, kk], at_dev.up).start()
            elif kind == "d":
                remote(dst, zu.at[s, k], z_s.at[s, k], zu_r.at[s, k], at_dev.down).start()

        each_of(group, body)

    def state_load(s):
        at = pl.ds(pl.multiple_of(s * rows, rows), rows)
        return [
            pltpu.make_async_copy(src.at[at], dst.at[at], st_ld.at[i, s])
            for i, (src, dst) in enumerate(((master, o_master), (mom1, o_mom1), (mom2, o_mom2)))
        ]

    def start_state(s):
        for copy in state_load(s):
            copy.start()

    def reduce_program(jobs, mid):
        ahead = 3
        for j in range(ahead):
            swap(jobs[j], j)
        prefetch(jobs[0], 0)
        for j, job in enumerate(jobs):
            if j + ahead < len(jobs):
                swap(jobs[j + ahead], j + ahead)
            if j + 1 < len(jobs):
                prefetch(jobs[j + 1], j + 1)
            run_job(job, j, mid)
            if j == len(jobs) // 2:
                each(0, STREAMS, start_state)

    nsum[...] = jnp.zeros_like(nsum)

    @pl.when(m == 0)
    def _():
        reduce_program(END_JOBS, False)

    @pl.when(m == 1)
    def _():
        reduce_program(MID_JOBS, True)

    def drain():
        block = acc.at[0, 0]

        @pl.when(m == 0)
        def _():
            for kind, u, qo, group in END_JOBS:
                if kind == "u":
                    each_of(group, lambda s: sent(block, z_s.at[s, 2 * u + qo]))
            each(0, STREAMS, lambda s: sent(block, q_s.at[s, 0]))

        @pl.when(m == 1)
        def _():
            for kind, u, qo, group in MID_JOBS:
                if kind == "u" or kind == "d":
                    each_of(group, lambda s: sent(block, z_s.at[s, 2 * u + qo]))

        each(0, 8 * STREAMS, lambda i: sent(block, first_s.at[i // 8, i % 8]))
        each(0, STREAMS, lambda s: sent(block, q_s.at[s, 1]))
        each(0, 16 * STREAMS, lambda i: core_copy(i // STREAMS, i % STREAMS).wait_send())

    def all_sum(part, place, count, others, slots, src, base, meanwhile=None):
        src[...] = part
        slots[place] = part
        for i, (other, _) in enumerate(others):
            remote(src, slots.at[place], norm_s.at[base + i], norm_r.at[base + place], other).start()
        if meanwhile is not None:
            meanwhile()
        for i, (_, slot) in enumerate(others):
            landed(slots.at[slot], norm_r.at[base + slot])
        total = slots[0]
        for i in range(1, count):
            total = total + slots[i]
        return total

    part = nsum[:, 0:128]
    for col in range(128, width, 128):
        part = part + nsum[:, col:col + 128]
    flat, z = at_dev.flat, at_dev.z
    part = all_sum(part, flat, 8, [(d, (flat + i + 1) % 8) for i, d in enumerate(at_dev.plane)], nr, nb.at[0], 0, drain)
    part = all_sum(part, z, 4, [(d, (z + i + 1) % 4) for i, d in enumerate(at_dev.zothers)], nz, nb.at[1], 8)
    square_sum = jnp.sum(part, keepdims=True)
    clip = jnp.minimum(1.0, 1.0 / (jnp.sqrt(square_sum) + 1e-6))
    clip = jnp.broadcast_to(clip, (tile, 128))

    learn_rate = lr_ref[0]
    inv1 = 1.0 / (1.0 - 0.9 ** ADAM_STEP)
    inv2 = 1.0 / (1.0 - 0.99 ** ADAM_STEP)
    decay_runs, fast_rows = rule_runs(width, total_rows)

    def update(s):
        for copy in state_load(s):
            copy.wait()

        def rows_step(t):
            base = pl.multiple_of(t * tile, tile)
            at = pl.ds(base, tile)
            out_at = pl.ds(pl.multiple_of(s * rows + t * tile, tile), tile)
            row = me * shard + s * rows + base + lax.broadcasted_iota(jnp.int32, (tile, 128), 0)
            decays = (row >= decay_runs[0][0]) & (row < decay_runs[0][1])
            for start, stop in decay_runs[1:]:
                decays = decays | ((row >= start) & (row < stop))
            fast = row == fast_rows[0]
            for fast_row in fast_rows[1:]:
                fast = fast | (row == fast_row)
            decay = jnp.where(decays, 0.1, 0.0)
            step_size = learn_rate * jnp.where(fast, 2.0, 1.0)
            for col in range(0, width, 128):
                cols = pl.ds(col, 128)
                g = acc[s, 2 * m, at, cols] * clip
                old = o_master[out_at, cols]
                first = 0.9 * o_mom1[out_at, cols] + 0.1 * g
                second = 0.99 * o_mom2[out_at, cols] + 0.01 * (g * g)
                new = old - step_size * ((first * inv1) / (jnp.sqrt(second * inv2) + 1e-8) + decay * old)
                o_master[out_at, cols] = new
                o_mom1[out_at, cols] = first
                o_mom2[out_at, cols] = second
                o_work[out_at, cols] = new.astype(jnp.bfloat16)

        each(0, rows // tile, rows_step)

    each(0, STREAMS, update)

    for i in range(7):
        sent(nb.at[0], norm_s.at[i])
    for i in range(3):
        sent(nb.at[1], norm_s.at[8 + i])


def gather_kernel(own_ref, o_work, own_s, gat_r, gcore_r, gcore_s, gp_s, gu_s, gd_s, gq_s):
    shard, width = own_ref.shape
    rows = shard // STREAMS
    at_dev = Place()
    me, c, m, chip = at_dev.me, at_dev.c, at_dev.m, at_dev.chip
    my_chip = me // 2

    enter([at_dev.partner, at_dev.xn, at_dev.yn] + at_dev.zothers)

    def work_rows(ci, s, cc):
        return o_work.at[pl.ds(pl.multiple_of((ci * 2 + cc) * shard + s * rows, rows), rows)]

    def send(src, ci, s, k, link):
        dst = work_rows(ci, s, c)
        i = ci * STREAMS + s
        if link == "c":
            remote(src, dst, gcore_s.at[i], gcore_r.at[i], at_dev.partner).start()
        else:
            to = {"p": at_dev.pn(s), "q": at_dev.qn(s), "u": at_dev.up, "d": at_dev.down}[link]
            ssem = {"p": gp_s, "q": gq_s, "u": gu_s, "d": gd_s}[link]
            remote(src, dst, ssem.at[s, k], gat_r.at[i], to).start()

    def gather_program(sends, own):
        first = [t for t in sends if t[:3] == own and t[4] == 0]

        def start_own(s):
            src = own_ref.at[pl.ds(pl.multiple_of(s * rows, rows), rows)]
            for u, qo, _, link, _ in first:
                send(src, my_chip, s, 2 * u + qo, link)

        each(0, STREAMS, start_own)

        def keep(t):
            at = pl.multiple_of(t * 32, 32)
            o_work[pl.ds(pl.multiple_of(me * shard + at, 32), 32), :] = own_ref[pl.ds(at, 32), :]

        each(0, shard // 32, keep)
        def settle(old):
            for (u, qo, _, link, group), n in old:
                def wait(s):
                    if link == "c":
                        ci = chip(s, u, qo, _)
                        ref = work_rows(ci, s, 1 - c)
                        i = ci * STREAMS + s
                        remote(ref, ref, gcore_s.at[i], gcore_r.at[i], me).wait()
                    else:
                        ssem = {"p": gp_s, "q": gq_s, "u": gu_s, "d": gd_s}[link]
                        remote(block_ref, block_ref, ssem.at[s, 2 * u + qo], gat_r.at[0], me).wait_send()

                each(group * GROUP, group * GROUP + GROUP, wait)

        block_ref = own_ref.at[pl.ds(0, rows)]
        rest = [t for t in sends if t[:3] != own]
        pending = [(t, -1) for t in sends if t[:3] == own]
        seen = set()
        n = 0
        while n < len(rest):
            block, group = rest[n][:3], rest[n][4]
            links = [rest[n][3]]
            start = n
            while n + 1 < len(rest) and rest[n + 1][:3] == block and rest[n + 1][4] == group:
                n += 1
                links.append(rest[n][3])
            n += 1
            new = (block, group) not in seen
            seen.add((block, group))
            if new:
                settle([p for p in pending if p[1] <= start - LAG])
                pending = [p for p in pending if p[1] > start - LAG]

            def body(s, block=block, links=tuple(links), new=new):
                ci = chip(s, *block)
                ref = work_rows(ci, s, c)
                if new:
                    remote(ref, ref, gcore_s.at[0], gat_r.at[ci * STREAMS + s], me).wait_recv()
                for link in links:
                    send(ref, ci, s, 2 * block[0] + block[1], link)

            each(group * GROUP, group * GROUP + GROUP, body)
            pending += [(t, start) for t in rest[start:n]]
        settle(pending)

    @pl.when(m == 0)
    def _():
        gather_program(END_SENDS, (0, 0, 0))

    @pl.when(m == 1)
    def _():
        gather_program(MID_SENDS, (1, 0, 0))


def store_kernel(*refs):
    ins, outs, sem = refs[:4], refs[4:8], refs[8]
    copies = [pltpu.make_async_copy(src, dst, sem.at[i]) for i, (src, dst) in enumerate(zip(ins[:3], outs[:3]))]
    pieces = sem.shape[0] - 3
    rows = ins[3].shape[0] // pieces
    for i in range(pieces):
        at = pl.ds(i * rows, rows)
        copies.append(pltpu.make_async_copy(ins[3].at[at], outs[3].at[at], sem.at[3 + i]))
    for copy in copies:
        copy.start()
    for copy in copies:
        copy.wait()


def solution(mesh):
    dev_count = mesh.shape["dp"]

    def device_step(local_grads, master, mom_first, mom_second, learn_rate):
        shard_rows, width = master.shape
        total_rows = shard_rows * dev_count
        rows = shard_rows // STREAMS
        any_spec = pl.BlockSpec(memory_space=pl.ANY)
        vmem_spec = pl.BlockSpec(memory_space=pltpu.VMEM)
        dma = pltpu.SemaphoreType.DMA
        f32, bf16 = jnp.float32, jnp.bfloat16
        shard = pltpu.VMEM((shard_rows, width), f32)
        new_master, new_first, new_second, own_rows, _ = pl.pallas_call(
            reduce_kernel,
            out_shape=[
                shard, shard, shard,
                pltpu.VMEM((shard_rows, width), bf16),
                jax.ShapeDtypeStruct((total_rows // 2, width), bf16),
            ],
            in_specs=[pl.BlockSpec(memory_space=pltpu.SMEM)] + [any_spec] * 4,
            out_specs=[vmem_spec] * 4 + [any_spec],
            scratch_shapes=[
                pltpu.VMEM((STREAMS, 8, rows, width), f32),
                pltpu.VMEM((STREAMS, 8, rows, width), f32),
                pltpu.VMEM((STREAMS, 5, rows, width), f32),
                pltpu.VMEM((STREAMS, 4, rows, width), f32),
                pltpu.VMEM((STREAMS, rows, width), f32),
                pltpu.VMEM((2, GROUP, 2, rows, width), bf16),
                pltpu.VMEM((8, width), f32),
                pltpu.VMEM((2, 8, 128), f32),
                pltpu.VMEM((8, 8, 128), f32),
                pltpu.VMEM((4, 8, 128), f32),
                dma((16 * STREAMS,)), dma((16 * STREAMS,)),
                dma((STREAMS, 8)), dma((STREAMS, 8)),
                dma((STREAMS, 8)), dma((STREAMS, 5)), dma((STREAMS, 4)),
                dma((STREAMS, 2)), dma((STREAMS,)), dma((STREAMS,)),
                dma((2, GROUP, 2)), dma((3, STREAMS)),
                dma((12,)), dma((12,)),
            ],
            compiler_params=pltpu.CompilerParams(
                collective_id=0, has_side_effects=True, vmem_limit_bytes=56 * 2 ** 20
            ),
            name="reduce_update",
        )(learn_rate.reshape(1), local_grads, master, mom_first, mom_second)
        working = pl.pallas_call(
            gather_kernel,
            out_shape=pltpu.VMEM((total_rows, width), bf16),
            in_specs=[vmem_spec],
            out_specs=vmem_spec,
            scratch_shapes=[
                dma((STREAMS,)), dma((16 * STREAMS,)), dma((16 * STREAMS,)), dma((16 * STREAMS,)),
                dma((STREAMS, 8)), dma((STREAMS, 8)), dma((STREAMS, 8)), dma((STREAMS, 8)),
            ],
            compiler_params=pltpu.CompilerParams(
                collective_id=1, has_side_effects=True, vmem_limit_bytes=4 * 2 ** 20
            ),
            name="gather_rows",
        )(own_rows)
        return pl.pallas_call(
            store_kernel,
            out_shape=[jax.ShapeDtypeStruct((shard_rows, width), f32)] * 3
            + [jax.ShapeDtypeStruct((total_rows, width), bf16)],
            in_specs=[vmem_spec] * 4,
            out_specs=[any_spec] * 4,
            scratch_shapes=[dma((3 + 32,))],
            compiler_params=pltpu.CompilerParams(vmem_limit_bytes=4 * 2 ** 20),
            name="store",
        )(new_master, new_first, new_second, working)

    return jax.shard_map(
        device_step,
        mesh=mesh,
        in_specs=(P("dp", None, None), P("dp", None), P("dp", None), P("dp", None), P()),
        out_specs=(P("dp", None), P("dp", None), P("dp", None), P(None, None)),
        check_vma=False,
    )
```

```python
import jax
import jax.numpy as jnp
from jax import lax
from jax.experimental import pallas as pl
from jax.experimental.pallas import tpu as pltpu
from jax.sharding import PartitionSpec as P

LAYERS = 2
MIX_RANK = 32
DECAY_RANK = 64
ADAM_STEP = 10
STREAMS = 8
GROUP = 4
LAG = 20
MESH = pl.DeviceIdType.MESH


def decode(codes):
    return [tuple(int(ch) if ch.isdigit() else ch for ch in code) for code in codes]


END_JOBS = decode([
    "f200", "f201", "u200", "f210", "f110", "f311", "u210", "f211", "f310", "u110", "u201", "p310",
    "p311", "f300", "f000", "u211", "f301", "f100", "u300", "f111", "f011", "u301", "u100", "n011",
    "f010", "f101", "u111", "n010", "u101", "f001", "r000", "r001",
])
MID_JOBS = decode([
    "f200", "f300", "f310", "f211", "f210", "f201", "u210", "f110", "f010", "u310", "f000", "u200",
    "f311", "u311", "f011", "d010", "u300", "f111", "u211", "f001", "d011", "f301", "d000", "n110",
    "f100", "u301", "f101", "u201", "d001", "n111", "r100", "r101",
])
END_SENDS = decode([
    "000q0", "000q1", "000u0", "000u1", "000p0", "000p1", "000c0", "000c1", "010p0", "100p0", "010u0", "200p0",
    "300p0", "100p1", "010u1", "300c0", "001c1", "010c1", "300p1", "100c0", "300q1", "011c0", "300q0", "010p1",
    "310c0", "200p1", "100c1", "110p0", "301c0", "301c1", "201c0", "101c1", "210p0", "010c0", "310p0", "210c0",
    "310p1", "110c0", "110p1", "310c1", "101c0", "201c1", "111c0", "200c0", "311c1", "311c0", "211c0", "200c1",
    "110c1", "011c1", "210p1", "001c0", "300c1", "210c1", "111c1", "211c1",
])
MID_SENDS = decode([
    "100q0", "100q1", "100u0", "100u1", "100d0", "100d1", "100p0", "100p1", "100c0", "100c1", "000u0", "000p0",
    "200d0", "000c1", "000p1", "200p0", "300d0", "000u1", "010p0", "110p1", "300d1", "300c1", "101c1", "110c0",
    "110d0", "010u0", "300c0", "300p1", "200c1", "200p1", "111c1", "110u0", "110p0", "010c0", "110c1", "310p0",
    "200d1", "001c0", "010c1", "111c0", "110u1", "101c0", "010u1", "300p0", "301c1", "310c0", "210d0", "210p0",
    "210c0", "210p1", "110d1", "210d1", "200c0", "210c1", "001c1", "311c0", "010p1", "011c0", "211c0", "301c0",
    "310p1", "211c1", "011c1", "000c0", "201c1", "310c1", "201c0", "311c1",
])


def rule_runs(model_width, total_rows):
    ffn_width = 7 * model_width // 2
    layer_rows = 6 * model_width + 2 * ffn_width + 16 + 10 * MIX_RANK + 2 * DECAY_RANK
    vocab_rows = (total_rows - LAYERS * layer_rows - 4) // 2
    decay_runs = [(0, vocab_rows)]
    fast_rows = []
    row = vocab_rows
    for layer_idx in range(LAYERS):
        row = row + (12 if layer_idx == 0 else 10) + 10 * MIX_RANK
        fast_rows.append(row)
        row = row + 1 + 2 * DECAY_RANK
        fast_rows.append(row)
        row = row + 1
        decay_runs.append((row, row + 5 * model_width))
        row = row + 5 * model_width + 4
        decay_runs.append((row, row + 2 * ffn_width + model_width))
        row = row + 2 * ffn_width + model_width
    row = row + 2
    decay_runs.append((row, row + vocab_rows))
    return decay_runs, fast_rows


def each(start, stop, body):
    def step(i, carry):
        body(i)
        return carry

    lax.fori_loop(start, stop, step, 0)


def remote(src, dst, ssem, rsem, to):
    return pltpu.make_async_remote_copy(
        src_ref=src, dst_ref=dst, send_sem=ssem, recv_sem=rsem, device_id=(to,), device_id_type=MESH
    )


class Place:
    def __init__(self):
        self.me = me = lax.axis_index("dp")
        self.c, self.x, self.y, self.z = c, x, y, z = me % 2, (me // 2) % 2, (me // 4) % 2, me // 8
        self.lo = 1 - z // 2
        self.m = self.lo * z + (1 - self.lo) * (3 - z)
        sgn = 2 * self.lo - 1
        self.partner = self.dev(z, y, x, 1 - c)
        self.xn, self.yn = self.dev(z, y, 1 - x, c), self.dev(z, 1 - y, x, c)
        self.up = self.dev(z + sgn, y, x, c)
        self.down = self.dev(z - sgn, y, x, c)
        self.flat = me % 8
        self.zothers = [((z + d) % 4) * 8 + self.flat for d in (1, 2, 3)]
        self.plane = [z * 8 + (self.flat + d) % 8 for d in range(1, 8)]

    def dev(self, zz, yy, xx, cc):
        return ((zz * 2 + yy) * 2 + xx) * 2 + cc

    def pn(self, s):
        h = s % 2
        return self.xn * (1 - h) + self.yn * h

    def qn(self, s):
        h = s % 2
        return self.yn * (1 - h) + self.xn * h

    def chip(self, s, u, qo, po):
        h = s % 2
        first = self.x * (1 - h) + self.y * h
        last = self.y * (1 - h) + self.x * h
        pv = 1 - first if po else first
        qv = 1 - last if qo else last
        xx = pv * (1 - h) + qv * h
        yy = qv * (1 - h) + pv * h
        return ((self.lo * u + (1 - self.lo) * (3 - u)) * 2 + yy) * 2 + xx


def enter(others):
    barrier = pltpu.get_barrier_semaphore()
    for other in others:
        pl.semaphore_signal(barrier, inc=1, device_id=(other,), device_id_type=MESH)
    pl.semaphore_wait(barrier, len(others))


def reduce_kernel(
    grads, o_grad, o_clip, praw,
    stg, acc, zd, zu, fin, rb, nsum, nb, nr, nz,
    core_s, core_r, first_s, first_r, z_s, zd_r, zu_r, q_s, pre_r, fin_r, ld, norm_s, norm_r,
):
    rows, width = acc.shape[2], acc.shape[3]
    shard = STREAMS * rows
    tile = min(32, rows)
    at_dev = Place()
    me, c, m, chip, pn, qn = at_dev.me, at_dev.c, at_dev.m, at_dev.chip, at_dev.pn, at_dev.qn

    enter(at_dev.plane + at_dev.zothers)

    def grad_rows(ci, s, cc):
        return grads.at[0, pl.ds(pl.multiple_of((ci * 2 + cc) * shard + s * rows, rows), rows)]

    def praw_rows(ci, s):
        return praw.at[pl.ds(pl.multiple_of((ci * STREAMS + s) * rows, rows), rows)]

    def core_copy(ci, s, dst=None):
        i = ci * STREAMS + s
        dst = praw_rows(ci, s) if dst is None else dst
        return remote(grad_rows(ci, s, 1 - c), dst, core_s.at[i], core_r.at[i], at_dev.partner)

    def each_of(group, body):
        each(group * GROUP, group * GROUP + GROUP, body)

    def loads(job, j, s):
        kind, u, qo, group = job
        ci = chip(s, u, qo, kind == "f")
        slot, i = j % 2, s - group * GROUP
        own = pltpu.make_async_copy(grad_rows(ci, s, c), rb.at[slot, i, 0], ld.at[slot, i, 0])
        if j < 2:
            return own, core_copy(ci, s, rb.at[slot, i, 1]), None
        return own, core_copy(ci, s), pltpu.make_async_copy(praw_rows(ci, s), rb.at[slot, i, 1], ld.at[slot, i, 1])

    def swap(job, j):
        each_of(job[3], lambda s: loads(job, j, s)[1].start())

    def prefetch(job, j):
        def body(s):
            own, core, other = loads(job, j, s)
            own.start()
            if other is not None:
                core.wait_recv()
                other.start()

        each_of(job[3], body)

    def landed(ref, rsem):
        remote(ref, ref, core_s.at[0], rsem, me).wait_recv()

    def sent(ref, ssem):
        remote(ref, ref, ssem, core_r.at[0], me).wait_send()

    def run_job(job, j, mid):
        kind, u, qo, group = job
        k = 2 * u + qo
        slot = j % 2

        def body(s):
            own, core, other = loads(job, j, s)
            parts = []
            if kind != "f":
                parts.append((acc.at[s, k], first_r.at[s, k]))
                if mid and u >= 1 and not (u == 3 and qo == 1):
                    parts.append((zd.at[s, k - 2], zd_r.at[s, k - 2]))
                if (mid and u <= 1) or (not mid and u == 0):
                    parts.append((zu.at[s, k], zu_r.at[s, k]))
                if not mid and (u, qo) == (3, 0):
                    parts.append((zd.at[s, 0], pre_r.at[s]))
                if kind == "r":
                    parts.append((fin.at[s], fin_r.at[s]))
            for ref, rsem in parts:
                landed(ref, rsem)
            own.wait()
            if other is None:
                core.wait_recv()
            else:
                other.wait()
            dst = stg.at[s, k] if kind == "f" else acc.at[s, k]
            if kind == "r":
                dst = o_grad.at[pl.ds(pl.multiple_of(s * rows, rows), rows)]
            i = s - group * GROUP

            def add(t):
                at = pl.ds(pl.multiple_of(t * tile, tile), tile)
                v = rb[slot, i, 0, at, :].astype(jnp.float32) + rb[slot, i, 1, at, :].astype(jnp.float32)
                for ref, _ in parts:
                    v = v + ref[at, :]
                if kind == "r":
                    v = v * (1.0 / 32.0)
                    nsum[...] += jnp.sum((v * v).reshape(tile // 8, 8, width), axis=0)
                dst[at, :] = v

            each(0, rows // tile, add)
            if kind == "f":
                remote(dst, acc.at[s, k], first_s.at[s, k], first_r.at[s, k], pn(s)).start()
            elif kind == "p":
                remote(dst, zd.at[s, 0], q_s.at[s, 0], pre_r.at[s], qn(s)).start()
            elif kind == "n":
                remote(dst, fin.at[s], q_s.at[s, 1], fin_r.at[s], qn(s)).start()
            elif kind == "u" and not mid:
                remote(dst, zd.at[s, k - 2], z_s.at[s, k], zd_r.at[s, k - 2], at_dev.up).start()
            elif kind == "u":
                kk = 2 * (3 - u) + qo
                remote(dst, zu.at[s, kk], z_s.at[s, k], zu_r.at[s, kk], at_dev.up).start()
            elif kind == "d":
                remote(dst, zu.at[s, k], z_s.at[s, k], zu_r.at[s, k], at_dev.down).start()

        each_of(group, body)

    def reduce_program(jobs, mid):
        ahead = 3
        for j in range(ahead):
            swap(jobs[j], j)
        prefetch(jobs[0], 0)
        for j, job in enumerate(jobs):
            if j + ahead < len(jobs):
                swap(jobs[j + ahead], j + ahead)
            if j + 1 < len(jobs):
                prefetch(jobs[j + 1], j + 1)
            run_job(job, j, mid)

    nsum[...] = jnp.zeros_like(nsum)

    @pl.when(m == 0)
    def _():
        reduce_program(END_JOBS, False)

    @pl.when(m == 1)
    def _():
        reduce_program(MID_JOBS, True)

    def drain():
        block = acc.at[0, 0]

        @pl.when(m == 0)
        def _():
            for kind, u, qo, group in END_JOBS:
                if kind == "u":
                    each_of(group, lambda s: sent(block, z_s.at[s, 2 * u + qo]))
            each(0, STREAMS, lambda s: sent(block, q_s.at[s, 0]))

        @pl.when(m == 1)
        def _():
            for kind, u, qo, group in MID_JOBS:
                if kind == "u" or kind == "d":
                    each_of(group, lambda s: sent(block, z_s.at[s, 2 * u + qo]))

        each(0, 8 * STREAMS, lambda i: sent(block, first_s.at[i // 8, i % 8]))
        each(0, STREAMS, lambda s: sent(block, q_s.at[s, 1]))
        each(0, 16 * STREAMS, lambda i: core_copy(i // STREAMS, i % STREAMS).wait_send())

    def all_sum(part, place, count, others, slots, src, base, meanwhile=None):
        src[...] = part
        slots[place] = part
        for i, (other, _) in enumerate(others):
            remote(src, slots.at[place], norm_s.at[base + i], norm_r.at[base + place], other).start()
        if meanwhile is not None:
            meanwhile()
        for i, (_, slot) in enumerate(others):
            landed(slots.at[slot], norm_r.at[base + slot])
        total = slots[0]
        for i in range(1, count):
            total = total + slots[i]
        return total

    part = nsum[:, 0:128]
    for col in range(128, width, 128):
        part = part + nsum[:, col:col + 128]
    flat, z = at_dev.flat, at_dev.z
    part = all_sum(part, flat, 8, [(d, (flat + i + 1) % 8) for i, d in enumerate(at_dev.plane)], nr, nb.at[0], 0, drain)
    part = all_sum(part, z, 4, [(d, (z + i + 1) % 4) for i, d in enumerate(at_dev.zothers)], nz, nb.at[1], 8)
    square_sum = jnp.sum(part, keepdims=True)
    clip = jnp.minimum(1.0, 1.0 / (jnp.sqrt(square_sum) + 1e-6))
    o_clip[...] = jnp.broadcast_to(clip, o_clip.shape)
    for i in range(7):
        sent(nb.at[0], norm_s.at[i])
    for i in range(3):
        sent(nb.at[1], norm_s.at[8 + i])


def gather_kernel(
    lr_ref, grad, clip_ref, master, mom1, mom2, o_master, o_mom1, o_mom2, o_work, st_ld, gat_r, gcore_r, gcore_s, gp_s, gu_s, gd_s, gq_s,
):
    shard, width = grad.shape
    total_rows = o_work.shape[0]
    rows = shard // STREAMS
    tile = min(32, rows)
    at_dev = Place()
    me, c, m, chip = at_dev.me, at_dev.c, at_dev.m, at_dev.chip
    my_chip = me // 2

    others = [at_dev.partner, at_dev.xn, at_dev.yn] + at_dev.zothers
    barrier = pltpu.get_barrier_semaphore()
    for other in others:
        pl.semaphore_signal(barrier, inc=1, device_id=(other,), device_id_type=MESH)

    def state_load(s):
        at = pl.ds(pl.multiple_of(s * rows, rows), rows)
        return [
            pltpu.make_async_copy(src.at[at], dst.at[at], st_ld.at[i, s])
            for i, (src, dst) in enumerate(((master, o_master), (mom1, o_mom1), (mom2, o_mom2)))
        ]

    def start_state(s):
        for copy in state_load(s):
            copy.start()

    each(0, STREAMS, start_state)

    learn_rate = lr_ref[0]
    inv1 = 1.0 / (1.0 - 0.9 ** ADAM_STEP)
    inv2 = 1.0 / (1.0 - 0.99 ** ADAM_STEP)
    decay_runs, fast_rows = rule_runs(width, total_rows)

    clip = jnp.broadcast_to(clip_ref[0:1, :], (tile, 128))

    def update(s):
        for copy in state_load(s):
            copy.wait()

        def rows_step(t):
            base = pl.multiple_of(t * tile, tile)
            out_at = pl.ds(pl.multiple_of(s * rows + t * tile, tile), tile)
            row = me * shard + s * rows + base + lax.broadcasted_iota(jnp.int32, (tile, 128), 0)
            decays = (row >= decay_runs[0][0]) & (row < decay_runs[0][1])
            for start, stop in decay_runs[1:]:
                decays = decays | ((row >= start) & (row < stop))
            fast = row == fast_rows[0]
            for fast_row in fast_rows[1:]:
                fast = fast | (row == fast_row)
            decay = jnp.where(decays, 0.1, 0.0)
            step_size = learn_rate * jnp.where(fast, 2.0, 1.0)
            for col in range(0, width, 128):
                cols = pl.ds(col, 128)
                g = grad[out_at, cols] * clip
                old = o_master[out_at, cols]
                first = 0.9 * o_mom1[out_at, cols] + 0.1 * g
                second = 0.99 * o_mom2[out_at, cols] + 0.01 * (g * g)
                new = old - step_size * ((first * inv1) / (jnp.sqrt(second * inv2) + 1e-8) + decay * old)
                o_master[out_at, cols] = new
                o_mom1[out_at, cols] = first
                o_mom2[out_at, cols] = second
                o_work[pl.ds(pl.multiple_of(me * shard + s * rows + base, tile), tile), cols] = new.astype(jnp.bfloat16)

        each(0, rows // tile, rows_step)

    update(0)
    pl.semaphore_wait(barrier, len(others))

    def work_rows(ci, s, cc):
        return o_work.at[pl.ds(pl.multiple_of((ci * 2 + cc) * shard + s * rows, rows), rows)]

    def send(src, ci, s, k, link):
        dst = work_rows(ci, s, c)
        i = ci * STREAMS + s
        if link == "c":
            remote(src, dst, gcore_s.at[i], gcore_r.at[i], at_dev.partner).start()
        else:
            to = {"p": at_dev.pn(s), "q": at_dev.qn(s), "u": at_dev.up, "d": at_dev.down}[link]
            ssem = {"p": gp_s, "q": gq_s, "u": gu_s, "d": gd_s}[link]
            remote(src, dst, ssem.at[s, k], gat_r.at[i], to).start()

    def gather_program(sends, own):
        first = [t for t in sends if t[:3] == own and t[4] == 0]

        def start_own(s):
            src = work_rows(my_chip, s, c)
            for u, qo, _, link, _ in first:
                send(src, my_chip, s, 2 * u + qo, link)

        start_own(0)

        def rest_own(s):
            update(s)
            start_own(s)

        each(1, STREAMS, rest_own)

        def settle(old):
            for (u, qo, _, link, group), n in old:
                def wait(s):
                    if link == "c":
                        ci = chip(s, u, qo, _)
                        ref = work_rows(ci, s, 1 - c)
                        i = ci * STREAMS + s
                        remote(ref, ref, gcore_s.at[i], gcore_r.at[i], me).wait()
                    else:
                        ssem = {"p": gp_s, "q": gq_s, "u": gu_s, "d": gd_s}[link]
                        remote(block_ref, block_ref, ssem.at[s, 2 * u + qo], gat_r.at[0], me).wait_send()

                each(group * GROUP, group * GROUP + GROUP, wait)

        block_ref = o_work.at[pl.ds(0, rows)]
        rest = [t for t in sends if t[:3] != own]
        pending = [(t, -1) for t in sends if t[:3] == own]
        seen = set()
        n = 0
        while n < len(rest):
            block, group = rest[n][:3], rest[n][4]
            links = [rest[n][3]]
            start = n
            while n + 1 < len(rest) and rest[n + 1][:3] == block and rest[n + 1][4] == group:
                n += 1
                links.append(rest[n][3])
            n += 1
            new = (block, group) not in seen
            seen.add((block, group))
            if new:
                settle([p for p in pending if p[1] <= start - LAG])
                pending = [p for p in pending if p[1] > start - LAG]

            def body(s, block=block, links=tuple(links), new=new):
                ci = chip(s, *block)
                ref = work_rows(ci, s, c)
                if new:
                    remote(ref, ref, gcore_s.at[0], gat_r.at[ci * STREAMS + s], me).wait_recv()
                for link in links:
                    send(ref, ci, s, 2 * block[0] + block[1], link)

            each(group * GROUP, group * GROUP + GROUP, body)
            pending += [(t, start) for t in rest[start:n]]
        settle(pending)

    @pl.when(m == 0)
    def _():
        gather_program(END_SENDS, (0, 0, 0))

    @pl.when(m == 1)
    def _():
        gather_program(MID_SENDS, (1, 0, 0))


def store_kernel(*refs):
    ins, outs, sem = refs[:4], refs[4:8], refs[8]
    copies = [pltpu.make_async_copy(src, dst, sem.at[i]) for i, (src, dst) in enumerate(zip(ins[:3], outs[:3]))]
    pieces = sem.shape[0] - 3
    rows = ins[3].shape[0] // pieces
    for i in range(pieces):
        at = pl.ds(i * rows, rows)
        copies.append(pltpu.make_async_copy(ins[3].at[at], outs[3].at[at], sem.at[3 + i]))
    for copy in copies:
        copy.start()
    for copy in copies:
        copy.wait()


def solution(mesh):
    dev_count = mesh.shape["dp"]

    def device_step(local_grads, master, mom_first, mom_second, learn_rate):
        shard_rows, width = master.shape
        total_rows = shard_rows * dev_count
        rows = shard_rows // STREAMS
        any_spec = pl.BlockSpec(memory_space=pl.ANY)
        vmem_spec = pl.BlockSpec(memory_space=pltpu.VMEM)
        hbm_spec = pl.BlockSpec(memory_space=pltpu.HBM)
        dma = pltpu.SemaphoreType.DMA
        f32, bf16 = jnp.float32, jnp.bfloat16
        shard = pltpu.VMEM((shard_rows, width), f32)
        grad_rows, clip, _ = pl.pallas_call(
            reduce_kernel,
            out_shape=[
                shard,
                pltpu.VMEM((8, 128), f32),
                jax.ShapeDtypeStruct((total_rows // 2, width), bf16),
            ],
            in_specs=[any_spec],
            out_specs=[vmem_spec] * 2 + [any_spec],
            scratch_shapes=[
                pltpu.VMEM((STREAMS, 8, rows, width), f32),
                pltpu.VMEM((STREAMS, 8, rows, width), f32),
                pltpu.VMEM((STREAMS, 5, rows, width), f32),
                pltpu.VMEM((STREAMS, 4, rows, width), f32),
                pltpu.VMEM((STREAMS, rows, width), f32),
                pltpu.VMEM((2, GROUP, 2, rows, width), bf16),
                pltpu.VMEM((8, width), f32),
                pltpu.VMEM((2, 8, 128), f32),
                pltpu.VMEM((8, 8, 128), f32),
                pltpu.VMEM((4, 8, 128), f32),
                dma((16 * STREAMS,)), dma((16 * STREAMS,)),
                dma((STREAMS, 8)), dma((STREAMS, 8)),
                dma((STREAMS, 8)), dma((STREAMS, 5)), dma((STREAMS, 4)),
                dma((STREAMS, 2)), dma((STREAMS,)), dma((STREAMS,)),
                dma((2, GROUP, 2)),
                dma((12,)), dma((12,)),
            ],
            compiler_params=pltpu.CompilerParams(
                collective_id=0, has_side_effects=True, vmem_limit_bytes=56 * 2 ** 20
            ),
            name="reduce_rows",
        )(local_grads)
        new_master, new_first, new_second, working = pl.pallas_call(
            gather_kernel,
            out_shape=[shard, shard, shard, pltpu.VMEM((total_rows, width), bf16)],
            in_specs=[pl.BlockSpec(memory_space=pltpu.SMEM)] + [vmem_spec] * 2 + [hbm_spec] * 3,
            out_specs=[vmem_spec] * 4,
            scratch_shapes=[
                dma((3, STREAMS)), dma((16 * STREAMS,)), dma((16 * STREAMS,)), dma((16 * STREAMS,)),
                dma((STREAMS, 8)), dma((STREAMS, 8)), dma((STREAMS, 8)), dma((STREAMS, 8)),
            ],
            compiler_params=pltpu.CompilerParams(
                collective_id=1, has_side_effects=True, vmem_limit_bytes=4 * 2 ** 20
            ),
            name="update_gather",
        )(learn_rate.reshape(1), grad_rows, clip, master, mom_first, mom_second)
        return pl.pallas_call(
            store_kernel,
            out_shape=[jax.ShapeDtypeStruct((shard_rows, width), f32)] * 3
            + [jax.ShapeDtypeStruct((total_rows, width), bf16)],
            in_specs=[vmem_spec] * 4,
            out_specs=[any_spec] * 4,
            scratch_shapes=[dma((3 + 32,))],
            compiler_params=pltpu.CompilerParams(vmem_limit_bytes=4 * 2 ** 20),
            name="store",
        )(new_master, new_first, new_second, working)

    return jax.shard_map(
        device_step,
        mesh=mesh,
        in_specs=(P("dp", None, None), P("dp", None), P("dp", None), P("dp", None), P()),
        out_specs=(P("dp", None), P("dp", None), P("dp", None), P(None, None)),
        check_vma=False,
    )
```

```python
import jax
import jax.numpy as jnp
from jax import lax
from jax.experimental import pallas as pl
from jax.experimental.pallas import tpu as pltpu
from jax.sharding import PartitionSpec as P

LAYERS = 2
MIX_RANK = 32
DECAY_RANK = 64
ADAM_STEP = 10
STREAMS = 8
GROUP = 4
LAG = 20
MESH = pl.DeviceIdType.MESH


def decode(codes):
    return [tuple(int(ch) if ch.isdigit() else ch for ch in code) for code in codes]


END_JOBS = decode([
    "f200", "f201", "u200", "f210", "f110", "f311", "u210", "f211", "f310", "u110", "u201", "p310",
    "p311", "f300", "f000", "u211", "f301", "f100", "u300", "f111", "f011", "u301", "u100", "n011",
    "f010", "f101", "u111", "n010", "u101", "f001", "r000", "r001",
])
MID_JOBS = decode([
    "f200", "f300", "f310", "f211", "f210", "f201", "u210", "f110", "f010", "u310", "f000", "u200",
    "f311", "u311", "f011", "d010", "u300", "f111", "u211", "f001", "d011", "f301", "d000", "n110",
    "f100", "u301", "f101", "u201", "d001", "n111", "r100", "r101",
])
END_SENDS = decode([
    "000q0", "000q1", "000u0", "000u1", "000p0", "000p1", "000c0", "000c1", "010p0", "100p0", "010u0", "200p0",
    "300p0", "100p1", "010u1", "300c0", "001c1", "010c1", "300p1", "100c0", "300q1", "011c0", "300q0", "010p1",
    "310c0", "200p1", "100c1", "110p0", "301c0", "301c1", "201c0", "101c1", "210p0", "010c0", "310p0", "210c0",
    "310p1", "110c0", "110p1", "310c1", "101c0", "201c1", "111c0", "200c0", "311c1", "311c0", "211c0", "200c1",
    "110c1", "011c1", "210p1", "001c0", "300c1", "210c1", "111c1", "211c1",
])
MID_SENDS = decode([
    "100q0", "100q1", "100u0", "100u1", "100d0", "100d1", "100p0", "100p1", "100c0", "100c1", "000u0", "000p0",
    "200d0", "000c1", "000p1", "200p0", "300d0", "000u1", "010p0", "110p1", "300d1", "300c1", "101c1", "110c0",
    "110d0", "010u0", "300c0", "300p1", "200c1", "200p1", "111c1", "110u0", "110p0", "010c0", "110c1", "310p0",
    "200d1", "001c0", "010c1", "111c0", "110u1", "101c0", "010u1", "300p0", "301c1", "310c0", "210d0", "210p0",
    "210c0", "210p1", "110d1", "210d1", "200c0", "210c1", "001c1", "311c0", "010p1", "011c0", "211c0", "301c0",
    "310p1", "211c1", "011c1", "000c0", "201c1", "310c1", "201c0", "311c1",
])


def rule_runs(model_width, total_rows):
    ffn_width = 7 * model_width // 2
    layer_rows = 6 * model_width + 2 * ffn_width + 16 + 10 * MIX_RANK + 2 * DECAY_RANK
    vocab_rows = (total_rows - LAYERS * layer_rows - 4) // 2
    decay_runs = [(0, vocab_rows)]
    fast_rows = []
    row = vocab_rows
    for layer_idx in range(LAYERS):
        row = row + (12 if layer_idx == 0 else 10) + 10 * MIX_RANK
        fast_rows.append(row)
        row = row + 1 + 2 * DECAY_RANK
        fast_rows.append(row)
        row = row + 1
        decay_runs.append((row, row + 5 * model_width))
        row = row + 5 * model_width + 4
        decay_runs.append((row, row + 2 * ffn_width + model_width))
        row = row + 2 * ffn_width + model_width
    row = row + 2
    decay_runs.append((row, row + vocab_rows))
    return decay_runs, fast_rows


def each(start, stop, body):
    def step(i, carry):
        body(i)
        return carry

    lax.fori_loop(start, stop, step, 0)


def remote(src, dst, ssem, rsem, to):
    return pltpu.make_async_remote_copy(
        src_ref=src, dst_ref=dst, send_sem=ssem, recv_sem=rsem, device_id=(to,), device_id_type=MESH
    )


class Place:
    def __init__(self):
        self.me = me = lax.axis_index("dp")
        self.c, self.x, self.y, self.z = c, x, y, z = me % 2, (me // 2) % 2, (me // 4) % 2, me // 8
        self.lo = 1 - z // 2
        self.m = self.lo * z + (1 - self.lo) * (3 - z)
        sgn = 2 * self.lo - 1
        self.partner = self.dev(z, y, x, 1 - c)
        self.xn, self.yn = self.dev(z, y, 1 - x, c), self.dev(z, 1 - y, x, c)
        self.up = self.dev(z + sgn, y, x, c)
        self.down = self.dev(z - sgn, y, x, c)
        self.flat = me % 8
        self.zothers = [((z + d) % 4) * 8 + self.flat for d in (1, 2, 3)]
        self.plane = [z * 8 + (self.flat + d) % 8 for d in range(1, 8)]

    def dev(self, zz, yy, xx, cc):
        return ((zz * 2 + yy) * 2 + xx) * 2 + cc

    def pn(self, s):
        if isinstance(s, int):
            return self.yn if s % 2 else self.xn
        h = s % 2
        return self.xn * (1 - h) + self.yn * h

    def qn(self, s):
        if isinstance(s, int):
            return self.xn if s % 2 else self.yn
        h = s % 2
        return self.yn * (1 - h) + self.xn * h

    def chip(self, s, u, qo, po):
        h = s % 2
        if isinstance(s, int):
            first, last = (self.y, self.x) if h else (self.x, self.y)
        else:
            first = self.x * (1 - h) + self.y * h
            last = self.y * (1 - h) + self.x * h
        pv = 1 - first if po else first
        qv = 1 - last if qo else last
        if isinstance(s, int):
            xx, yy = (qv, pv) if s % 2 else (pv, qv)
            return ((self.lo * u + (1 - self.lo) * (3 - u)) * 2 + yy) * 2 + xx
        xx = pv * (1 - h) + qv * h
        yy = qv * (1 - h) + pv * h
        return ((self.lo * u + (1 - self.lo) * (3 - u)) * 2 + yy) * 2 + xx


def enter(others):
    barrier = pltpu.get_barrier_semaphore()
    for other in others:
        pl.semaphore_signal(barrier, inc=1, device_id=(other,), device_id_type=MESH)
    pl.semaphore_wait(barrier, len(others))


def reduce_kernel(
    grads, o_grad, o_clip, praw,
    stg, acc, zd, zu, fin, rb, nsum, nb, nr, nz,
    core_s, core_r, first_s, first_r, z_s, zd_r, zu_r, q_s, pre_r, fin_r, ld, norm_s, norm_r,
):
    rows, width = acc.shape[2], acc.shape[3]
    shard = STREAMS * rows
    tile = min(32, rows)
    at_dev = Place()
    me, c, m, chip, pn, qn = at_dev.me, at_dev.c, at_dev.m, at_dev.chip, at_dev.pn, at_dev.qn

    enter(at_dev.plane + at_dev.zothers)

    def grad_rows(ci, s, cc):
        return grads.at[0, pl.ds(pl.multiple_of((ci * 2 + cc) * shard + s * rows, rows), rows)]

    def praw_rows(ci, s):
        return praw.at[pl.ds(pl.multiple_of((ci * STREAMS + s) * rows, rows), rows)]

    def core_copy(ci, s, dst=None):
        i = ci * STREAMS + s
        dst = praw_rows(ci, s) if dst is None else dst
        return remote(grad_rows(ci, s, 1 - c), dst, core_s.at[i], core_r.at[i], at_dev.partner)

    def each_of(group, body):
        each(group * GROUP, group * GROUP + GROUP, body)

    def loads(job, j, s):
        kind, u, qo, group = job
        ci = chip(s, u, qo, kind == "f")
        slot, i = j % 2, s - group * GROUP
        own = pltpu.make_async_copy(grad_rows(ci, s, c), rb.at[slot, i, 0], ld.at[slot, i, 0])
        if j < 2:
            return own, core_copy(ci, s, rb.at[slot, i, 1]), None
        return own, core_copy(ci, s), pltpu.make_async_copy(praw_rows(ci, s), rb.at[slot, i, 1], ld.at[slot, i, 1])

    def swap(job, j):
        each_of(job[3], lambda s: loads(job, j, s)[1].start())

    def prefetch(job, j):
        def body(s):
            own, core, other = loads(job, j, s)
            own.start()
            if other is not None:
                core.wait_recv()
                other.start()

        each_of(job[3], body)

    def landed(ref, rsem):
        remote(ref, ref, core_s.at[0], rsem, me).wait_recv()

    def sent(ref, ssem):
        remote(ref, ref, ssem, core_r.at[0], me).wait_send()

    def run_job(job, j, mid):
        kind, u, qo, group = job
        k = 2 * u + qo
        slot = j % 2

        def body(s):
            own, core, other = loads(job, j, s)
            parts = []
            if kind != "f":
                parts.append((acc.at[s, k], first_r.at[s, k]))
                if mid and u >= 1 and not (u == 3 and qo == 1):
                    parts.append((zd.at[s, k - 2], zd_r.at[s, k - 2]))
                if (mid and u <= 1) or (not mid and u == 0):
                    parts.append((zu.at[s, k], zu_r.at[s, k]))
                if not mid and (u, qo) == (3, 0):
                    parts.append((zd.at[s, 0], pre_r.at[s]))
                if kind == "r":
                    parts.append((fin.at[s], fin_r.at[s]))
            for ref, rsem in parts:
                landed(ref, rsem)
            own.wait()
            if other is None:
                core.wait_recv()
            else:
                other.wait()
            dst = stg.at[s, k] if kind == "f" else acc.at[s, k]
            if kind == "r":
                dst = o_grad.at[pl.ds(pl.multiple_of(s * rows, rows), rows)]
            i = s - group * GROUP

            def add(t):
                at = pl.ds(pl.multiple_of(t * tile, tile), tile)
                v = rb[slot, i, 0, at, :].astype(jnp.float32) + rb[slot, i, 1, at, :].astype(jnp.float32)
                for ref, _ in parts:
                    v = v + ref[at, :]
                if kind == "r":
                    v = v * (1.0 / 32.0)
                    nsum[...] += jnp.sum((v * v).reshape(tile // 8, 8, width), axis=0)
                dst[at, :] = v

            each(0, rows // tile, add)
            if kind == "f":
                remote(dst, acc.at[s, k], first_s.at[s, k], first_r.at[s, k], pn(s)).start()
            elif kind == "p":
                remote(dst, zd.at[s, 0], q_s.at[s, 0], pre_r.at[s], qn(s)).start()
            elif kind == "n":
                remote(dst, fin.at[s], q_s.at[s, 1], fin_r.at[s], qn(s)).start()
            elif kind == "u" and not mid:
                remote(dst, zd.at[s, k - 2], z_s.at[s, k], zd_r.at[s, k - 2], at_dev.up).start()
            elif kind == "u":
                kk = 2 * (3 - u) + qo
                remote(dst, zu.at[s, kk], z_s.at[s, k], zu_r.at[s, kk], at_dev.up).start()
            elif kind == "d":
                remote(dst, zu.at[s, k], z_s.at[s, k], zu_r.at[s, k], at_dev.down).start()

        each_of(group, body)

    def reduce_program(jobs, mid):
        ahead = 3
        for j in range(ahead):
            swap(jobs[j], j)
        prefetch(jobs[0], 0)
        for j, job in enumerate(jobs):
            if j + ahead < len(jobs):
                swap(jobs[j + ahead], j + ahead)
            if j + 1 < len(jobs):
                prefetch(jobs[j + 1], j + 1)
            run_job(job, j, mid)

    nsum[...] = jnp.zeros_like(nsum)

    @pl.when(m == 0)
    def _():
        reduce_program(END_JOBS, False)

    @pl.when(m == 1)
    def _():
        reduce_program(MID_JOBS, True)

    def drain():
        block = acc.at[0, 0]

        @pl.when(m == 0)
        def _():
            for kind, u, qo, group in END_JOBS:
                if kind == "u":
                    each_of(group, lambda s: sent(block, z_s.at[s, 2 * u + qo]))
            each(0, STREAMS, lambda s: sent(block, q_s.at[s, 0]))

        @pl.when(m == 1)
        def _():
            for kind, u, qo, group in MID_JOBS:
                if kind == "u" or kind == "d":
                    each_of(group, lambda s: sent(block, z_s.at[s, 2 * u + qo]))

        each(0, 8 * STREAMS, lambda i: sent(block, first_s.at[i // 8, i % 8]))
        each(0, STREAMS, lambda s: sent(block, q_s.at[s, 1]))
        each(0, 16 * STREAMS, lambda i: core_copy(i // STREAMS, i % STREAMS).wait_send())

    def all_sum(part, place, count, others, slots, src, base, meanwhile=None):
        src[...] = part
        slots[place] = part
        for i, (other, _) in enumerate(others):
            remote(src, slots.at[place], norm_s.at[base + i], norm_r.at[base + place], other).start()
        if meanwhile is not None:
            meanwhile()
        for i, (_, slot) in enumerate(others):
            landed(slots.at[slot], norm_r.at[base + slot])
        total = slots[0]
        for i in range(1, count):
            total = total + slots[i]
        return total

    part = nsum[:, 0:128]
    for col in range(128, width, 128):
        part = part + nsum[:, col:col + 128]
    flat, z = at_dev.flat, at_dev.z
    part = all_sum(part, flat, 8, [(d, (flat + i + 1) % 8) for i, d in enumerate(at_dev.plane)], nr, nb.at[0], 0, drain)
    part = all_sum(part, z, 4, [(d, (z + i + 1) % 4) for i, d in enumerate(at_dev.zothers)], nz, nb.at[1], 8)
    square_sum = jnp.sum(part, keepdims=True)
    clip = jnp.minimum(1.0, 1.0 / (jnp.sqrt(square_sum) + 1e-6))
    o_clip[...] = jnp.broadcast_to(clip, o_clip.shape)
    for i in range(7):
        sent(nb.at[0], norm_s.at[i])
    for i in range(3):
        sent(nb.at[1], norm_s.at[8 + i])


def gather_kernel(
    lr_ref, grad, clip_ref, master, mom1, mom2, o_master, o_mom1, o_mom2, o_work, gat_r, gcore_r, gcore_s, gp_s, gu_s, gd_s, gq_s,
):
    shard, width = grad.shape
    total_rows = o_work.shape[0]
    rows = shard // STREAMS
    tile = min(32, rows)
    at_dev = Place()
    me, c, m, chip = at_dev.me, at_dev.c, at_dev.m, at_dev.chip
    my_chip = me // 2

    others = [at_dev.partner, at_dev.xn, at_dev.yn] + at_dev.zothers
    barrier = pltpu.get_barrier_semaphore()
    for other in others:
        pl.semaphore_signal(barrier, inc=1, device_id=(other,), device_id_type=MESH)

    learn_rate = lr_ref[0]
    inv1 = 1.0 / (1.0 - 0.9 ** ADAM_STEP)
    inv2 = 1.0 / (1.0 - 0.99 ** ADAM_STEP)
    decay_runs, fast_rows = rule_runs(width, total_rows)

    clip = jnp.broadcast_to(clip_ref[0:1, :], (tile, 128))

    def update(s):
        def rows_step(t):
            base = pl.multiple_of(t * tile, tile)
            out_at = pl.ds(pl.multiple_of(s * rows + t * tile, tile), tile)
            row = me * shard + s * rows + base + lax.broadcasted_iota(jnp.int32, (tile, 128), 0)
            decays = (row >= decay_runs[0][0]) & (row < decay_runs[0][1])
            for start, stop in decay_runs[1:]:
                decays = decays | ((row >= start) & (row < stop))
            fast = row == fast_rows[0]
            for fast_row in fast_rows[1:]:
                fast = fast | (row == fast_row)
            decay = jnp.where(decays, 0.1, 0.0)
            step_size = learn_rate * jnp.where(fast, 2.0, 1.0)
            for col in range(0, width, 128):
                cols = pl.ds(col, 128)
                g = grad[out_at, cols] * clip
                old = master[out_at, cols]
                first = 0.9 * mom1[out_at, cols] + 0.1 * g
                second = 0.99 * mom2[out_at, cols] + 0.01 * (g * g)
                new = old - step_size * ((first * inv1) / (jnp.sqrt(second * inv2) + 1e-8) + decay * old)
                o_master[out_at, cols] = new
                o_mom1[out_at, cols] = first
                o_mom2[out_at, cols] = second
                o_work[pl.ds(pl.multiple_of(me * shard + s * rows + base, tile), tile), cols] = new.astype(jnp.bfloat16)

        each(0, rows // tile, rows_step)

    update(0)
    pl.semaphore_wait(barrier, len(others))

    def work_rows(ci, s, cc):
        return o_work.at[pl.ds(pl.multiple_of((ci * 2 + cc) * shard + s * rows, rows), rows)]

    def send(src, ci, s, k, link):
        dst = work_rows(ci, s, c)
        i = ci * STREAMS + s
        if link == "c":
            remote(src, dst, gcore_s.at[i], gcore_r.at[i], at_dev.partner).start()
        else:
            to = {"p": at_dev.pn(s), "q": at_dev.qn(s), "u": at_dev.up, "d": at_dev.down}[link]
            ssem = {"p": gp_s, "q": gq_s, "u": gu_s, "d": gd_s}[link]
            remote(src, dst, ssem.at[s, k], gat_r.at[i], to).start()

    def gather_program(sends, own):
        first = [t for t in sends if t[:3] == own and t[4] == 0]

        def start_own(s):
            src = work_rows(my_chip, s, c)
            for u, qo, _, link, _ in first:
                send(src, my_chip, s, 2 * u + qo, link)

        start_own(0)

        def rest_own(s):
            update(s)
            start_own(s)

        each(1, STREAMS, rest_own)

        def settle(old):
            for (u, qo, _, link, group), n in old:
                def wait(s):
                    if link == "c":
                        ci = chip(s, u, qo, _)
                        ref = work_rows(ci, s, 1 - c)
                        i = ci * STREAMS + s
                        remote(ref, ref, gcore_s.at[i], gcore_r.at[i], me).wait()
                    else:
                        ssem = {"p": gp_s, "q": gq_s, "u": gu_s, "d": gd_s}[link]
                        remote(block_ref, block_ref, ssem.at[s, 2 * u + qo], gat_r.at[0], me).wait_send()

                each(group * GROUP, group * GROUP + GROUP, wait)

        block_ref = o_work.at[pl.ds(0, rows)]
        rest = [t for t in sends if t[:3] != own]
        pending = [(t, -1) for t in sends if t[:3] == own]
        seen = set()
        n = 0
        while n < len(rest):
            block, group = rest[n][:3], rest[n][4]
            links = [rest[n][3]]
            start = n
            while n + 1 < len(rest) and rest[n + 1][:3] == block and rest[n + 1][4] == group:
                n += 1
                links.append(rest[n][3])
            n += 1
            new = (block, group) not in seen
            seen.add((block, group))
            if new:
                settle([p for p in pending if p[1] <= start - LAG])
                pending = [p for p in pending if p[1] > start - LAG]

            def body(s, block=block, links=tuple(links), new=new):
                ci = chip(s, *block)
                ref = work_rows(ci, s, c)
                if new:
                    remote(ref, ref, gcore_s.at[0], gat_r.at[ci * STREAMS + s], me).wait_recv()
                for link in links:
                    send(ref, ci, s, 2 * block[0] + block[1], link)

            for s in range(group * GROUP, group * GROUP + GROUP):
                body(s)
            pending += [(t, start) for t in rest[start:n]]
        settle(pending)

    @pl.when(m == 0)
    def _():
        gather_program(END_SENDS, (0, 0, 0))

    @pl.when(m == 1)
    def _():
        gather_program(MID_SENDS, (1, 0, 0))


def store_kernel(*refs):
    ins, outs, sem = refs[:4], refs[4:8], refs[8]
    copies = [pltpu.make_async_copy(src, dst, sem.at[i]) for i, (src, dst) in enumerate(zip(ins[:3], outs[:3]))]
    pieces = sem.shape[0] - 3
    rows = ins[3].shape[0] // pieces
    for i in range(pieces):
        at = pl.ds(i * rows, rows)
        copies.append(pltpu.make_async_copy(ins[3].at[at], outs[3].at[at], sem.at[3 + i]))
    for copy in copies:
        copy.start()
    for copy in copies:
        copy.wait()


def solution(mesh):
    dev_count = mesh.shape["dp"]

    def device_step(local_grads, master, mom_first, mom_second, learn_rate):
        shard_rows, width = master.shape
        total_rows = shard_rows * dev_count
        rows = shard_rows // STREAMS
        any_spec = pl.BlockSpec(memory_space=pl.ANY)
        vmem_spec = pl.BlockSpec(memory_space=pltpu.VMEM)
        dma = pltpu.SemaphoreType.DMA
        f32, bf16 = jnp.float32, jnp.bfloat16
        shard = pltpu.VMEM((shard_rows, width), f32)
        grad_rows, clip, _ = pl.pallas_call(
            reduce_kernel,
            out_shape=[
                shard,
                pltpu.VMEM((8, 128), f32),
                jax.ShapeDtypeStruct((total_rows // 2, width), bf16),
            ],
            in_specs=[any_spec],
            out_specs=[vmem_spec] * 2 + [any_spec],
            scratch_shapes=[
                pltpu.VMEM((STREAMS, 8, rows, width), f32),
                pltpu.VMEM((STREAMS, 8, rows, width), f32),
                pltpu.VMEM((STREAMS, 5, rows, width), f32),
                pltpu.VMEM((STREAMS, 4, rows, width), f32),
                pltpu.VMEM((STREAMS, rows, width), f32),
                pltpu.VMEM((2, GROUP, 2, rows, width), bf16),
                pltpu.VMEM((8, width), f32),
                pltpu.VMEM((2, 8, 128), f32),
                pltpu.VMEM((8, 8, 128), f32),
                pltpu.VMEM((4, 8, 128), f32),
                dma((16 * STREAMS,)), dma((16 * STREAMS,)),
                dma((STREAMS, 8)), dma((STREAMS, 8)),
                dma((STREAMS, 8)), dma((STREAMS, 5)), dma((STREAMS, 4)),
                dma((STREAMS, 2)), dma((STREAMS,)), dma((STREAMS,)),
                dma((2, GROUP, 2)),
                dma((12,)), dma((12,)),
            ],
            compiler_params=pltpu.CompilerParams(
                collective_id=0, has_side_effects=True, vmem_limit_bytes=217 * 2 ** 18
            ),
            name="reduce_rows",
        )(local_grads)
        new_master, new_first, new_second, working = pl.pallas_call(
            gather_kernel,
            out_shape=[shard, shard, shard, pltpu.VMEM((total_rows, width), bf16)],
            in_specs=[pl.BlockSpec(memory_space=pltpu.SMEM)] + [vmem_spec] * 5,
            out_specs=[vmem_spec] * 4,
            scratch_shapes=[
                dma((16 * STREAMS,)), dma((16 * STREAMS,)), dma((16 * STREAMS,)),
                dma((STREAMS, 8)), dma((STREAMS, 8)), dma((STREAMS, 8)), dma((STREAMS, 8)),
            ],
            compiler_params=pltpu.CompilerParams(
                collective_id=1, has_side_effects=True, vmem_limit_bytes=4 * 2 ** 20
            ),
            name="update_gather",
        )(learn_rate.reshape(1), grad_rows, clip, master, mom_first, mom_second)
        return pl.pallas_call(
            store_kernel,
            out_shape=[jax.ShapeDtypeStruct((shard_rows, width), f32)] * 3
            + [jax.ShapeDtypeStruct((total_rows, width), bf16)],
            in_specs=[vmem_spec] * 4,
            out_specs=[any_spec] * 4,
            scratch_shapes=[dma((3 + 32,))],
            compiler_params=pltpu.CompilerParams(vmem_limit_bytes=4 * 2 ** 20),
            name="store",
        )(new_master, new_first, new_second, working)

    return jax.shard_map(
        device_step,
        mesh=mesh,
        in_specs=(P("dp", None, None), P("dp", None), P("dp", None), P("dp", None), P()),
        out_specs=(P("dp", None), P("dp", None), P("dp", None), P(None, None)),
        check_vma=False,
    )
```

```python
import jax
import jax.numpy as jnp
from jax import lax
from jax.experimental import pallas as pl
from jax.experimental.pallas import tpu as pltpu
from jax.sharding import PartitionSpec as P

LAYERS = 2
MIX_RANK = 32
DECAY_RANK = 64
ADAM_STEP = 10
STREAMS = 8
GROUP = 4
LAG = 20
MESH = pl.DeviceIdType.MESH


def decode(codes):
    return [tuple(int(ch) if ch.isdigit() else ch for ch in code) for code in codes]


END_JOBS = decode([
    "f200", "f211", "u200", "f201", "u211", "f210", "f110", "u210", "f310", "f300", "u110", "f311",
    "f100", "p310", "u201", "f301", "u300", "f111", "p311", "u111", "f000", "u301", "f011", "f101",
    "u100", "f010", "n010", "n011", "f001", "u101", "r000", "r001",
])
MID_JOBS = decode([
    "f301", "f211", "f311", "f110", "f210", "f310", "f300", "f011", "u211", "f201", "u310", "f010",
    "u311", "u210", "f200", "f001", "d010", "f000", "f101", "u300", "u200", "d000", "f100", "f111",
    "d011", "n110", "u301", "d001", "u201", "n111", "r100", "r101",
])
END_SENDS = decode([
    "000q0", "000q1", "000u0", "000u1", "000p0", "000p1", "000c0", "000c1", "010p0", "100p0", "010u0", "200p0",
    "300p0", "100p1", "010u1", "300c0", "001c1", "010c1", "300p1", "100c0", "300q1", "011c0", "300q0", "010p1",
    "310c0", "200p1", "100c1", "110p0", "301c0", "301c1", "201c0", "101c1", "210p0", "010c0", "310p0", "210c0",
    "310p1", "110c0", "110p1", "310c1", "101c0", "201c1", "111c0", "200c0", "311c1", "311c0", "211c0", "200c1",
    "110c1", "011c1", "210p1", "001c0", "300c1", "210c1", "111c1", "211c1",
])
MID_SENDS = decode([
    "100q0", "100q1", "100u0", "100u1", "100d0", "100d1", "100p0", "100p1", "100c0", "100c1", "000u0", "000p0",
    "200d0", "000c1", "000p1", "200p0", "300d0", "000u1", "010p0", "110p1", "300d1", "300c1", "101c1", "110c0",
    "110d0", "010u0", "300c0", "300p1", "200c1", "200p1", "111c1", "110u0", "110p0", "010c0", "110c1", "310p0",
    "200d1", "001c0", "010c1", "111c0", "110u1", "101c0", "010u1", "300p0", "301c1", "310c0", "210d0", "210p0",
    "210c0", "210p1", "110d1", "210d1", "200c0", "210c1", "001c1", "311c0", "010p1", "011c0", "211c0", "301c0",
    "310p1", "211c1", "011c1", "000c0", "201c1", "310c1", "201c0", "311c1",
])


def rule_runs(model_width, total_rows):
    ffn_width = 7 * model_width // 2
    layer_rows = 6 * model_width + 2 * ffn_width + 16 + 10 * MIX_RANK + 2 * DECAY_RANK
    vocab_rows = (total_rows - LAYERS * layer_rows - 4) // 2
    decay_runs = [(0, vocab_rows)]
    fast_rows = []
    row = vocab_rows
    for layer_idx in range(LAYERS):
        row = row + (12 if layer_idx == 0 else 10) + 10 * MIX_RANK
        fast_rows.append(row)
        row = row + 1 + 2 * DECAY_RANK
        fast_rows.append(row)
        row = row + 1
        decay_runs.append((row, row + 5 * model_width))
        row = row + 5 * model_width + 4
        decay_runs.append((row, row + 2 * ffn_width + model_width))
        row = row + 2 * ffn_width + model_width
    row = row + 2
    decay_runs.append((row, row + vocab_rows))
    return decay_runs, fast_rows


def each(start, stop, body):
    def step(i, carry):
        body(i)
        return carry

    lax.fori_loop(start, stop, step, 0)


def remote(src, dst, ssem, rsem, to):
    return pltpu.make_async_remote_copy(
        src_ref=src, dst_ref=dst, send_sem=ssem, recv_sem=rsem, device_id=(to,), device_id_type=MESH
    )


class Place:
    def __init__(self):
        self.me = me = lax.axis_index("dp")
        self.c, self.x, self.y, self.z = c, x, y, z = me % 2, (me // 2) % 2, (me // 4) % 2, me // 8
        self.lo = 1 - z // 2
        self.m = self.lo * z + (1 - self.lo) * (3 - z)
        sgn = 2 * self.lo - 1
        self.partner = self.dev(z, y, x, 1 - c)
        self.xn, self.yn = self.dev(z, y, 1 - x, c), self.dev(z, 1 - y, x, c)
        self.up = self.dev(z + sgn, y, x, c)
        self.down = self.dev(z - sgn, y, x, c)
        self.flat = me % 8
        self.zothers = [((z + d) % 4) * 8 + self.flat for d in (1, 2, 3)]
        self.plane = [z * 8 + (self.flat + d) % 8 for d in range(1, 8)]

    def dev(self, zz, yy, xx, cc):
        return ((zz * 2 + yy) * 2 + xx) * 2 + cc

    def pn(self, s):
        if isinstance(s, int):
            return self.yn if s % 2 else self.xn
        h = s % 2
        return self.xn * (1 - h) + self.yn * h

    def qn(self, s):
        if isinstance(s, int):
            return self.xn if s % 2 else self.yn
        h = s % 2
        return self.yn * (1 - h) + self.xn * h

    def chip(self, s, u, qo, po):
        h = s % 2
        if isinstance(s, int):
            first, last = (self.y, self.x) if h else (self.x, self.y)
        else:
            first = self.x * (1 - h) + self.y * h
            last = self.y * (1 - h) + self.x * h
        pv = 1 - first if po else first
        qv = 1 - last if qo else last
        if isinstance(s, int):
            xx, yy = (qv, pv) if s % 2 else (pv, qv)
            return ((self.lo * u + (1 - self.lo) * (3 - u)) * 2 + yy) * 2 + xx
        xx = pv * (1 - h) + qv * h
        yy = qv * (1 - h) + pv * h
        return ((self.lo * u + (1 - self.lo) * (3 - u)) * 2 + yy) * 2 + xx


def enter(others):
    barrier = pltpu.get_barrier_semaphore()
    for other in others:
        pl.semaphore_signal(barrier, inc=1, device_id=(other,), device_id_type=MESH)
    pl.semaphore_wait(barrier, len(others))


def reduce_kernel(
    grads, o_grad, o_clip, praw,
    stg, acc, zd, zu, fin, rb, nsum, nb, nr, nz,
    core_s, core_r, first_s, first_r, half_r, z_s, zd_r, zu_r, q_s, pre_r, fin_r, ld, norm_s, norm_r,
):
    rows, width = acc.shape[2], acc.shape[3]
    shard = STREAMS * rows
    tile = min(32, rows // 2)
    at_dev = Place()
    me, c, m, chip, pn, qn = at_dev.me, at_dev.c, at_dev.m, at_dev.chip, at_dev.pn, at_dev.qn

    enter(at_dev.plane + at_dev.zothers)

    def grad_rows(ci, s, cc):
        return grads.at[0, pl.ds(pl.multiple_of((ci * 2 + cc) * shard + s * rows, rows), rows)]

    def praw_rows(ci, s):
        return praw.at[pl.ds(pl.multiple_of((ci * STREAMS + s) * rows, rows), rows)]

    def core_copy(ci, s, dst=None):
        i = ci * STREAMS + s
        dst = praw_rows(ci, s) if dst is None else dst
        return remote(grad_rows(ci, s, 1 - c), dst, core_s.at[i], core_r.at[i], at_dev.partner)

    def each_of(group, body):
        each(group * GROUP, group * GROUP + GROUP, body)

    def loads(job, j, s):
        kind, u, qo, group = job
        ci = chip(s, u, qo, kind == "f")
        slot, i = j % 2, s - group * GROUP
        own = pltpu.make_async_copy(grad_rows(ci, s, c), rb.at[slot, i, 0], ld.at[slot, i, 0])
        if j < 2:
            return own, core_copy(ci, s, rb.at[slot, i, 1]), None
        return own, core_copy(ci, s), pltpu.make_async_copy(praw_rows(ci, s), rb.at[slot, i, 1], ld.at[slot, i, 1])

    def swap(job, j):
        each_of(job[3], lambda s: loads(job, j, s)[1].start())

    def prefetch(job, j):
        def body(s):
            own, core, other = loads(job, j, s)
            own.start()
            if other is not None:
                core.wait_recv()
                other.start()

        each_of(job[3], body)

    def landed(ref, rsem):
        remote(ref, ref, core_s.at[0], rsem, me).wait_recv()

    def sent(ref, ssem):
        remote(ref, ref, ssem, core_r.at[0], me).wait_send()

    def run_job(job, j, mid):
        kind, u, qo, group = job
        k = 2 * u + qo
        slot = j % 2
        early = not mid and job[1:] == END_JOBS[0][1:]
        pieces = 2 if early and kind in ("f", "u") else 1
        size = rows // pieces

        def body(s):
            own, core, other = loads(job, j, s)
            parts = []
            if kind != "f":
                parts.append((acc.at[s, k], first_r.at[s, k]))
                if mid and u >= 1 and not (u == 3 and qo == 1):
                    parts.append((zd.at[s, k - 2], zd_r.at[s, k - 2]))
                if (mid and u <= 1) or (not mid and u == 0):
                    parts.append((zu.at[s, k], zu_r.at[s, k]))
                if not mid and (u, qo) == (3, 0):
                    parts.append((zd.at[s, 0], pre_r.at[s]))
                if kind == "r":
                    parts.append((fin.at[s], fin_r.at[s]))
            dst = stg.at[s, k] if kind == "f" else acc.at[s, k]
            if kind == "r":
                dst = o_grad.at[pl.ds(pl.multiple_of(s * rows, rows), rows)]
            i = s - group * GROUP

            def add(t):
                at = pl.ds(pl.multiple_of(t * tile, tile), tile)
                v = rb[slot, i, 0, at, :].astype(jnp.float32) + rb[slot, i, 1, at, :].astype(jnp.float32)
                for ref, _ in parts:
                    v = v + ref[at, :]
                if kind == "r":
                    v = v * (1.0 / 32.0)
                    nsum[...] += jnp.sum((v * v).reshape(tile // 8, 8, width), axis=0)
                dst[at, :] = v

            for piece in range(pieces):
                cut = pl.ds(piece * size, size)
                for n, (ref, rsem) in enumerate(parts):
                    if n == 0 and early:
                        landed(ref.at[cut], half_r.at[s] if piece else rsem)
                    elif piece == 0:
                        landed(ref, rsem)
                if piece == 0:
                    own.wait()
                    if other is None:
                        core.wait_recv()
                    else:
                        other.wait()
                each(piece * size // tile, (piece + 1) * size // tile, add)
                src = dst.at[cut]
                if kind == "f":
                    rsem = half_r.at[s] if piece else first_r.at[s, k]
                    remote(src, acc.at[s, k].at[cut], first_s.at[s, k], rsem, pn(s)).start()
                elif kind == "p":
                    remote(src, zd.at[s, 0], q_s.at[s, 0], pre_r.at[s], qn(s)).start()
                elif kind == "n":
                    remote(src, fin.at[s], q_s.at[s, 1], fin_r.at[s], qn(s)).start()
                elif kind == "u" and not mid:
                    remote(src, zd.at[s, k - 2].at[cut], z_s.at[s, k], zd_r.at[s, k - 2], at_dev.up).start()
                elif kind == "u":
                    kk = 2 * (3 - u) + qo
                    remote(src, zu.at[s, kk], z_s.at[s, k], zu_r.at[s, kk], at_dev.up).start()
                elif kind == "d":
                    remote(src, zu.at[s, k], z_s.at[s, k], zu_r.at[s, k], at_dev.down).start()

        each_of(group, body)

    def reduce_program(jobs, mid):
        ahead = 3
        for j in range(ahead):
            swap(jobs[j], j)
        prefetch(jobs[0], 0)
        for j, job in enumerate(jobs):
            if j + ahead < len(jobs):
                swap(jobs[j + ahead], j + ahead)
            if j + 1 < len(jobs):
                prefetch(jobs[j + 1], j + 1)
            run_job(job, j, mid)

    nsum[...] = jnp.zeros_like(nsum)

    @pl.when(m == 0)
    def _():
        reduce_program(END_JOBS, False)

    @pl.when(m == 1)
    def _():
        reduce_program(MID_JOBS, True)

    def drain():
        block = acc.at[0, 0]

        @pl.when(m == 0)
        def _():
            for kind, u, qo, group in END_JOBS:
                if kind == "u":
                    each_of(group, lambda s: sent(block, z_s.at[s, 2 * u + qo]))
            each(0, STREAMS, lambda s: sent(block, q_s.at[s, 0]))

        @pl.when(m == 1)
        def _():
            for kind, u, qo, group in MID_JOBS:
                if kind == "u" or kind == "d":
                    each_of(group, lambda s: sent(block, z_s.at[s, 2 * u + qo]))

        each(0, 8 * STREAMS, lambda i: sent(block, first_s.at[i // 8, i % 8]))
        each(0, STREAMS, lambda s: sent(block, q_s.at[s, 1]))
        each(0, 16 * STREAMS, lambda i: core_copy(i // STREAMS, i % STREAMS).wait_send())

    def all_sum(part, place, count, others, slots, src, base, meanwhile=None):
        src[...] = part
        slots[place] = part
        for i, (other, _) in enumerate(others):
            remote(src, slots.at[place], norm_s.at[base + i], norm_r.at[base + place], other).start()
        if meanwhile is not None:
            meanwhile()
        for i, (_, slot) in enumerate(others):
            landed(slots.at[slot], norm_r.at[base + slot])
        total = slots[0]
        for i in range(1, count):
            total = total + slots[i]
        return total

    part = nsum[:, 0:128]
    for col in range(128, width, 128):
        part = part + nsum[:, col:col + 128]
    flat, z = at_dev.flat, at_dev.z
    part = all_sum(part, flat, 8, [(d, (flat + i + 1) % 8) for i, d in enumerate(at_dev.plane)], nr, nb.at[0], 0, drain)
    part = all_sum(part, z, 4, [(d, (z + i + 1) % 4) for i, d in enumerate(at_dev.zothers)], nz, nb.at[1], 8)
    square_sum = jnp.sum(part, keepdims=True)
    clip = jnp.minimum(1.0, 1.0 / (jnp.sqrt(square_sum) + 1e-6))
    o_clip[...] = jnp.broadcast_to(clip, o_clip.shape)
    for i in range(7):
        sent(nb.at[0], norm_s.at[i])
    for i in range(3):
        sent(nb.at[1], norm_s.at[8 + i])


def gather_kernel(
    lr_ref, grad, clip_ref, master, mom1, mom2, o_master, o_mom1, o_mom2, o_work, gat_r, gcore_r, gcore_s, gp_s, gu_s, gd_s, gq_s,
):
    shard, width = grad.shape
    total_rows = o_work.shape[0]
    rows = shard // STREAMS
    tile = min(32, rows)
    at_dev = Place()
    me, c, m, chip = at_dev.me, at_dev.c, at_dev.m, at_dev.chip
    my_chip = me // 2

    others = [at_dev.partner, at_dev.xn, at_dev.yn] + at_dev.zothers
    barrier = pltpu.get_barrier_semaphore()
    for other in others:
        pl.semaphore_signal(barrier, inc=1, device_id=(other,), device_id_type=MESH)

    learn_rate = lr_ref[0]
    inv1 = 1.0 / (1.0 - 0.9 ** ADAM_STEP)
    inv2 = 1.0 / (1.0 - 0.99 ** ADAM_STEP)
    decay_runs, fast_rows = rule_runs(width, total_rows)

    clip = jnp.broadcast_to(clip_ref[0:1, :], (tile, 128))

    def update(s):
        def rows_step(t):
            base = pl.multiple_of(t * tile, tile)
            out_at = pl.ds(pl.multiple_of(s * rows + t * tile, tile), tile)
            row = me * shard + s * rows + base + lax.broadcasted_iota(jnp.int32, (tile, 128), 0)
            decays = (row >= decay_runs[0][0]) & (row < decay_runs[0][1])
            for start, stop in decay_runs[1:]:
                decays = decays | ((row >= start) & (row < stop))
            fast = row == fast_rows[0]
            for fast_row in fast_rows[1:]:
                fast = fast | (row == fast_row)
            decay = jnp.where(decays, 0.1, 0.0)
            step_size = learn_rate * jnp.where(fast, 2.0, 1.0)
            for col in range(0, width, 128):
                cols = pl.ds(col, 128)
                g = grad[out_at, cols] * clip
                old = master[out_at, cols]
                first = 0.9 * mom1[out_at, cols] + 0.1 * g
                second = 0.99 * mom2[out_at, cols] + 0.01 * (g * g)
                new = old - step_size * ((first * inv1) / (jnp.sqrt(second * inv2) + 1e-8) + decay * old)
                o_master[out_at, cols] = new
                o_mom1[out_at, cols] = first
                o_mom2[out_at, cols] = second
                o_work[pl.ds(pl.multiple_of(me * shard + s * rows + base, tile), tile), cols] = new.astype(jnp.bfloat16)

        each(0, rows // tile, rows_step)

    update(0)
    pl.semaphore_wait(barrier, len(others))

    def work_rows(ci, s, cc):
        return o_work.at[pl.ds(pl.multiple_of((ci * 2 + cc) * shard + s * rows, rows), rows)]

    def send(src, ci, s, k, link):
        dst = work_rows(ci, s, c)
        i = ci * STREAMS + s
        if link == "c":
            remote(src, dst, gcore_s.at[i], gcore_r.at[i], at_dev.partner).start()
        else:
            to = {"p": at_dev.pn(s), "q": at_dev.qn(s), "u": at_dev.up, "d": at_dev.down}[link]
            ssem = {"p": gp_s, "q": gq_s, "u": gu_s, "d": gd_s}[link]
            remote(src, dst, ssem.at[s, k], gat_r.at[i], to).start()

    def gather_program(sends, own):
        first = [t for t in sends if t[:3] == own and t[4] == 0]

        def start_own(s):
            src = work_rows(my_chip, s, c)
            for u, qo, _, link, _ in first:
                send(src, my_chip, s, 2 * u + qo, link)

        start_own(0)

        def rest_own(s):
            update(s)
            start_own(s)

        each(1, STREAMS, rest_own)

        def settle(old):
            for (u, qo, _, link, group), n in old:
                def wait(s):
                    if link == "c":
                        ci = chip(s, u, qo, _)
                        ref = work_rows(ci, s, 1 - c)
                        i = ci * STREAMS + s
                        remote(ref, ref, gcore_s.at[i], gcore_r.at[i], me).wait()
                    else:
                        ssem = {"p": gp_s, "q": gq_s, "u": gu_s, "d": gd_s}[link]
                        remote(block_ref, block_ref, ssem.at[s, 2 * u + qo], gat_r.at[0], me).wait_send()

                each(group * GROUP, group * GROUP + GROUP, wait)

        block_ref = o_work.at[pl.ds(0, rows)]
        rest = [t for t in sends if t[:3] != own]
        pending = [(t, -1) for t in sends if t[:3] == own]
        seen = set()
        n = 0
        while n < len(rest):
            block, group = rest[n][:3], rest[n][4]
            links = [rest[n][3]]
            start = n
            while n + 1 < len(rest) and rest[n + 1][:3] == block and rest[n + 1][4] == group:
                n += 1
                links.append(rest[n][3])
            n += 1
            new = (block, group) not in seen
            seen.add((block, group))
            if new:
                settle([p for p in pending if p[1] <= start - LAG])
                pending = [p for p in pending if p[1] > start - LAG]

            def body(s, block=block, links=tuple(links), new=new):
                ci = chip(s, *block)
                ref = work_rows(ci, s, c)
                if new:
                    remote(ref, ref, gcore_s.at[0], gat_r.at[ci * STREAMS + s], me).wait_recv()
                for link in links:
                    send(ref, ci, s, 2 * block[0] + block[1], link)

            for s in range(group * GROUP, group * GROUP + GROUP):
                body(s)
            pending += [(t, start) for t in rest[start:n]]
        settle(pending)

    @pl.when(m == 0)
    def _():
        gather_program(END_SENDS, (0, 0, 0))

    @pl.when(m == 1)
    def _():
        gather_program(MID_SENDS, (1, 0, 0))


def store_kernel(*refs):
    ins, outs, sem = refs[:4], refs[4:8], refs[8]
    copies = [pltpu.make_async_copy(src, dst, sem.at[i]) for i, (src, dst) in enumerate(zip(ins[:3], outs[:3]))]
    pieces = sem.shape[0] - 3
    rows = ins[3].shape[0] // pieces
    for i in range(pieces):
        at = pl.ds(i * rows, rows)
        copies.append(pltpu.make_async_copy(ins[3].at[at], outs[3].at[at], sem.at[3 + i]))
    for copy in copies:
        copy.start()
    for copy in copies:
        copy.wait()


def solution(mesh):
    dev_count = mesh.shape["dp"]

    def device_step(local_grads, master, mom_first, mom_second, learn_rate):
        shard_rows, width = master.shape
        total_rows = shard_rows * dev_count
        rows = shard_rows // STREAMS
        any_spec = pl.BlockSpec(memory_space=pl.ANY)
        vmem_spec = pl.BlockSpec(memory_space=pltpu.VMEM)
        dma = pltpu.SemaphoreType.DMA
        f32, bf16 = jnp.float32, jnp.bfloat16
        shard = pltpu.VMEM((shard_rows, width), f32)
        grad_rows, clip, _ = pl.pallas_call(
            reduce_kernel,
            out_shape=[
                shard,
                pltpu.VMEM((8, 128), f32),
                jax.ShapeDtypeStruct((total_rows // 2, width), bf16),
            ],
            in_specs=[any_spec],
            out_specs=[vmem_spec] * 2 + [any_spec],
            scratch_shapes=[
                pltpu.VMEM((STREAMS, 8, rows, width), f32),
                pltpu.VMEM((STREAMS, 8, rows, width), f32),
                pltpu.VMEM((STREAMS, 5, rows, width), f32),
                pltpu.VMEM((STREAMS, 4, rows, width), f32),
                pltpu.VMEM((STREAMS, rows, width), f32),
                pltpu.VMEM((2, GROUP, 2, rows, width), bf16),
                pltpu.VMEM((8, width), f32),
                pltpu.VMEM((2, 8, 128), f32),
                pltpu.VMEM((8, 8, 128), f32),
                pltpu.VMEM((4, 8, 128), f32),
                dma((16 * STREAMS,)), dma((16 * STREAMS,)),
                dma((STREAMS, 8)), dma((STREAMS, 8)), dma((STREAMS,)),
                dma((STREAMS, 8)), dma((STREAMS, 5)), dma((STREAMS, 4)),
                dma((STREAMS, 2)), dma((STREAMS,)), dma((STREAMS,)),
                dma((2, GROUP, 2)),
                dma((12,)), dma((12,)),
            ],
            compiler_params=pltpu.CompilerParams(
                collective_id=0, has_side_effects=True, vmem_limit_bytes=217 * 2 ** 18
            ),
            name="reduce_rows",
        )(local_grads)
        new_master, new_first, new_second, working = pl.pallas_call(
            gather_kernel,
            out_shape=[shard, shard, shard, pltpu.VMEM((total_rows, width), bf16)],
            in_specs=[pl.BlockSpec(memory_space=pltpu.SMEM)] + [vmem_spec] * 5,
            out_specs=[vmem_spec] * 4,
            scratch_shapes=[
                dma((16 * STREAMS,)), dma((16 * STREAMS,)), dma((16 * STREAMS,)),
                dma((STREAMS, 8)), dma((STREAMS, 8)), dma((STREAMS, 8)), dma((STREAMS, 8)),
            ],
            compiler_params=pltpu.CompilerParams(
                collective_id=1, has_side_effects=True, vmem_limit_bytes=4 * 2 ** 20
            ),
            name="update_gather",
        )(learn_rate.reshape(1), grad_rows, clip, master, mom_first, mom_second)
        return pl.pallas_call(
            store_kernel,
            out_shape=[jax.ShapeDtypeStruct((shard_rows, width), f32)] * 3
            + [jax.ShapeDtypeStruct((total_rows, width), bf16)],
            in_specs=[vmem_spec] * 4,
            out_specs=[any_spec] * 4,
            scratch_shapes=[dma((3 + 8,))],
            compiler_params=pltpu.CompilerParams(vmem_limit_bytes=4 * 2 ** 20),
            name="store",
        )(new_master, new_first, new_second, working)

    return jax.shard_map(
        device_step,
        mesh=mesh,
        in_specs=(P("dp", None, None), P("dp", None), P("dp", None), P("dp", None), P()),
        out_specs=(P("dp", None), P("dp", None), P("dp", None), P(None, None)),
        check_vma=False,
    )
```

```python
import jax
import jax.numpy as jnp
from jax import lax
from jax.experimental import pallas as pl
from jax.experimental.pallas import tpu as pltpu
from jax.sharding import PartitionSpec as P

LAYERS = 2
MIX_RANK = 32
DECAY_RANK = 64
ADAM_STEP = 10
STREAMS = 8
GROUP = 4
LAG = 20
MESH = pl.DeviceIdType.MESH


def decode(codes):
    return [tuple(int(ch) if ch.isdigit() else ch for ch in code) for code in codes]


END_JOBS = decode([
    "f200", "f211", "u200", "f201", "u211", "f210", "f110", "u210", "f310", "f300", "u110", "f311",
    "f100", "p310", "u201", "f301", "u300", "f111", "p311", "u111", "f000", "u301", "f011", "f101",
    "u100", "f010", "n010", "n011", "f001", "u101", "r000", "r001",
])
MID_JOBS = decode([
    "f301", "f211", "f311", "f110", "f210", "f310", "f300", "f011", "u211", "f201", "u310", "f010",
    "u311", "u210", "f200", "f001", "d010", "f000", "f101", "u300", "u200", "d000", "f100", "f111",
    "d011", "n110", "u301", "d001", "u201", "n111", "r100", "r101",
])
END_SENDS = decode([
    "000q0", "000q1", "000u0", "000u1", "000p0", "000p1", "000c0", "000c1", "010p0", "100p0", "010u0", "200p0",
    "300p0", "100p1", "010u1", "300c0", "001c1", "010c1", "300p1", "100c0", "300q1", "011c0", "300q0", "010p1",
    "310c0", "200p1", "100c1", "110p0", "301c0", "301c1", "201c0", "101c1", "210p0", "010c0", "310p0", "210c0",
    "310p1", "110c0", "110p1", "310c1", "101c0", "201c1", "111c0", "200c0", "311c1", "311c0", "211c0", "200c1",
    "110c1", "011c1", "210p1", "001c0", "300c1", "210c1", "111c1", "211c1",
])
MID_SENDS = decode([
    "100q0", "100q1", "100u0", "100u1", "100d0", "100d1", "100p0", "100p1", "100c0", "100c1", "000u0", "000p0",
    "200d0", "000c1", "000p1", "200p0", "300d0", "000u1", "010p0", "110p1", "300d1", "300c1", "101c1", "110c0",
    "110d0", "010u0", "300c0", "300p1", "200c1", "200p1", "111c1", "110u0", "110p0", "010c0", "110c1", "310p0",
    "200d1", "001c0", "010c1", "111c0", "110u1", "101c0", "010u1", "300p0", "301c1", "310c0", "210d0", "210p0",
    "210c0", "210p1", "110d1", "210d1", "200c0", "210c1", "001c1", "311c0", "010p1", "011c0", "211c0", "301c0",
    "310p1", "211c1", "011c1", "000c0", "201c1", "310c1", "201c0", "311c1",
])


def rule_runs(model_width, total_rows):
    ffn_width = 7 * model_width // 2
    layer_rows = 6 * model_width + 2 * ffn_width + 16 + 10 * MIX_RANK + 2 * DECAY_RANK
    vocab_rows = (total_rows - LAYERS * layer_rows - 4) // 2
    decay_runs = [(0, vocab_rows)]
    fast_rows = []
    row = vocab_rows
    for layer_idx in range(LAYERS):
        row = row + (12 if layer_idx == 0 else 10) + 10 * MIX_RANK
        fast_rows.append(row)
        row = row + 1 + 2 * DECAY_RANK
        fast_rows.append(row)
        row = row + 1
        decay_runs.append((row, row + 5 * model_width))
        row = row + 5 * model_width + 4
        decay_runs.append((row, row + 2 * ffn_width + model_width))
        row = row + 2 * ffn_width + model_width
    row = row + 2
    decay_runs.append((row, row + vocab_rows))
    return decay_runs, fast_rows


def each(start, stop, body):
    def step(i, carry):
        body(i)
        return carry

    lax.fori_loop(start, stop, step, 0)


def remote(src, dst, ssem, rsem, to):
    return pltpu.make_async_remote_copy(
        src_ref=src, dst_ref=dst, send_sem=ssem, recv_sem=rsem, device_id=(to,), device_id_type=MESH
    )


class Place:
    def __init__(self):
        self.me = me = lax.axis_index("dp")
        self.c, self.x, self.y, self.z = c, x, y, z = me % 2, (me // 2) % 2, (me // 4) % 2, me // 8
        self.lo = 1 - z // 2
        self.m = self.lo * z + (1 - self.lo) * (3 - z)
        sgn = 2 * self.lo - 1
        self.partner = self.dev(z, y, x, 1 - c)
        self.xn, self.yn = self.dev(z, y, 1 - x, c), self.dev(z, 1 - y, x, c)
        self.up = self.dev(z + sgn, y, x, c)
        self.down = self.dev(z - sgn, y, x, c)
        self.flat = me % 8
        self.zothers = [((z + d) % 4) * 8 + self.flat for d in (1, 2, 3)]
        self.plane = [z * 8 + (self.flat + d) % 8 for d in range(1, 8)]

    def dev(self, zz, yy, xx, cc):
        return ((zz * 2 + yy) * 2 + xx) * 2 + cc

    def pn(self, s):
        if isinstance(s, int):
            return self.yn if s % 2 else self.xn
        h = s % 2
        return self.xn * (1 - h) + self.yn * h

    def qn(self, s):
        if isinstance(s, int):
            return self.xn if s % 2 else self.yn
        h = s % 2
        return self.yn * (1 - h) + self.xn * h

    def chip(self, s, u, qo, po):
        h = s % 2
        if isinstance(s, int):
            first, last = (self.y, self.x) if h else (self.x, self.y)
        else:
            first = self.x * (1 - h) + self.y * h
            last = self.y * (1 - h) + self.x * h
        pv = 1 - first if po else first
        qv = 1 - last if qo else last
        if isinstance(s, int):
            xx, yy = (qv, pv) if s % 2 else (pv, qv)
            return ((self.lo * u + (1 - self.lo) * (3 - u)) * 2 + yy) * 2 + xx
        xx = pv * (1 - h) + qv * h
        yy = qv * (1 - h) + pv * h
        return ((self.lo * u + (1 - self.lo) * (3 - u)) * 2 + yy) * 2 + xx


def enter(others):
    barrier = pltpu.get_barrier_semaphore()
    for other in others:
        pl.semaphore_signal(barrier, inc=1, device_id=(other,), device_id_type=MESH)
    pl.semaphore_wait(barrier, len(others))


def reduce_kernel(
    grads, o_grad, o_clip, praw,
    stg, acc, zd, zu, fin, rb, nsum, nb, nr, nz,
    core_s, core_r, first_s, first_r, half_r, z_s, zd_r, zu_r, q_s, pre_r, fin_r, ld, norm_s, norm_r,
):
    rows, width = acc.shape[2], acc.shape[3]
    shard = STREAMS * rows
    tile = min(32, rows // 2)
    at_dev = Place()
    me, c, m, chip, pn, qn = at_dev.me, at_dev.c, at_dev.m, at_dev.chip, at_dev.pn, at_dev.qn

    enter(at_dev.plane + at_dev.zothers)

    def grad_rows(ci, s, cc):
        return grads.at[0, pl.ds(pl.multiple_of((ci * 2 + cc) * shard + s * rows, rows), rows)]

    def praw_rows(ci, s):
        return praw.at[pl.ds(pl.multiple_of((ci * STREAMS + s) * rows, rows), rows)]

    def core_copy(ci, s, dst=None):
        i = ci * STREAMS + s
        dst = praw_rows(ci, s) if dst is None else dst
        return remote(grad_rows(ci, s, 1 - c), dst, core_s.at[i], core_r.at[i], at_dev.partner)

    def each_of(group, body):
        each(group * GROUP, group * GROUP + GROUP, body)

    def loads(job, j, s):
        kind, u, qo, group = job
        ci = chip(s, u, qo, kind == "f")
        slot, i = j % 2, s - group * GROUP
        own = pltpu.make_async_copy(grad_rows(ci, s, c), rb.at[slot, i, 0], ld.at[slot, i, 0])
        if j < 2:
            return own, core_copy(ci, s, rb.at[slot, i, 1]), None
        return own, core_copy(ci, s), pltpu.make_async_copy(praw_rows(ci, s), rb.at[slot, i, 1], ld.at[slot, i, 1])

    def swap(job, j):
        each_of(job[3], lambda s: loads(job, j, s)[1].start())

    def prefetch(job, j):
        def body(s):
            own, core, other = loads(job, j, s)
            own.start()
            if other is not None:
                core.wait_recv()
                other.start()

        each_of(job[3], body)

    def landed(ref, rsem):
        remote(ref, ref, core_s.at[0], rsem, me).wait_recv()

    def sent(ref, ssem):
        remote(ref, ref, ssem, core_r.at[0], me).wait_send()

    def run_job(job, j, mid):
        kind, u, qo, group = job
        k = 2 * u + qo
        slot = j % 2
        early = not mid and job[1:] == END_JOBS[0][1:]
        pieces = 2 if early and kind in ("f", "u") else 1
        size = rows // pieces

        def body(s):
            own, core, other = loads(job, j, s)
            parts = []
            if kind != "f":
                parts.append((acc.at[s, k], first_r.at[s, k]))
                if mid and u >= 1 and not (u == 3 and qo == 1):
                    parts.append((zd.at[s, k - 2], zd_r.at[s, k - 2]))
                if (mid and u <= 1) or (not mid and u == 0):
                    parts.append((zu.at[s, k], zu_r.at[s, k]))
                if not mid and (u, qo) == (3, 0):
                    parts.append((zd.at[s, 0], pre_r.at[s]))
                if kind == "r":
                    parts.append((fin.at[s], fin_r.at[s]))
            dst = stg.at[s, k] if kind == "f" else acc.at[s, k]
            if kind == "r":
                dst = o_grad.at[pl.ds(pl.multiple_of(s * rows, rows), rows)]
            i = s - group * GROUP

            def add(t):
                at = pl.ds(pl.multiple_of(t * tile, tile), tile)
                v = rb[slot, i, 0, at, :].astype(jnp.float32) + rb[slot, i, 1, at, :].astype(jnp.float32)
                for ref, _ in parts:
                    v = v + ref[at, :]
                if kind == "r":
                    v = v * (1.0 / 32.0)
                    nsum[...] += jnp.sum((v * v).reshape(tile // 8, 8, width), axis=0)
                dst[at, :] = v

            for piece in range(pieces):
                cut = pl.ds(piece * size, size)
                for n, (ref, rsem) in enumerate(parts):
                    if n == 0 and early:
                        landed(ref.at[cut], half_r.at[s] if piece else rsem)
                    elif piece == 0:
                        landed(ref, rsem)
                if piece == 0:
                    own.wait()
                    if other is None:
                        core.wait_recv()
                    else:
                        other.wait()
                each(piece * size // tile, (piece + 1) * size // tile, add)
                src = dst.at[cut]
                if kind == "f":
                    rsem = half_r.at[s] if piece else first_r.at[s, k]
                    remote(src, acc.at[s, k].at[cut], first_s.at[s, k], rsem, pn(s)).start()
                elif kind == "p":
                    remote(src, zd.at[s, 0], q_s.at[s, 0], pre_r.at[s], qn(s)).start()
                elif kind == "n":
                    remote(src, fin.at[s], q_s.at[s, 1], fin_r.at[s], qn(s)).start()
                elif kind == "u" and not mid:
                    remote(src, zd.at[s, k - 2].at[cut], z_s.at[s, k], zd_r.at[s, k - 2], at_dev.up).start()
                elif kind == "u":
                    kk = 2 * (3 - u) + qo
                    remote(src, zu.at[s, kk], z_s.at[s, k], zu_r.at[s, kk], at_dev.up).start()
                elif kind == "d":
                    remote(src, zu.at[s, k], z_s.at[s, k], zu_r.at[s, k], at_dev.down).start()

        each_of(group, body)

    def reduce_program(jobs, mid):
        ahead = 3
        for j in range(ahead):
            swap(jobs[j], j)
        prefetch(jobs[0], 0)
        for j, job in enumerate(jobs):
            if j + ahead < len(jobs):
                swap(jobs[j + ahead], j + ahead)
            if j + 1 < len(jobs):
                prefetch(jobs[j + 1], j + 1)
            run_job(job, j, mid)

    nsum[...] = jnp.zeros_like(nsum)

    @pl.when(m == 0)
    def _():
        reduce_program(END_JOBS, False)

    @pl.when(m == 1)
    def _():
        reduce_program(MID_JOBS, True)

    def drain():
        block = acc.at[0, 0]

        @pl.when(m == 0)
        def _():
            for kind, u, qo, group in END_JOBS:
                if kind == "u":
                    each_of(group, lambda s: sent(block, z_s.at[s, 2 * u + qo]))
            each(0, STREAMS, lambda s: sent(block, q_s.at[s, 0]))

        @pl.when(m == 1)
        def _():
            for kind, u, qo, group in MID_JOBS:
                if kind == "u" or kind == "d":
                    each_of(group, lambda s: sent(block, z_s.at[s, 2 * u + qo]))

        each(0, 8 * STREAMS, lambda i: sent(block, first_s.at[i // 8, i % 8]))
        each(0, STREAMS, lambda s: sent(block, q_s.at[s, 1]))
        each(0, 16 * STREAMS, lambda i: core_copy(i // STREAMS, i % STREAMS).wait_send())

    def all_sum(part, place, count, others, slots, src, base, meanwhile=None):
        src[...] = part
        slots[place] = part
        for i, (other, _) in enumerate(others):
            remote(src, slots.at[place], norm_s.at[base + i], norm_r.at[base + place], other).start()
        if meanwhile is not None:
            meanwhile()
        for i, (_, slot) in enumerate(others):
            landed(slots.at[slot], norm_r.at[base + slot])
        total = slots[0]
        for i in range(1, count):
            total = total + slots[i]
        return total

    part = nsum[:, 0:128]
    for col in range(128, width, 128):
        part = part + nsum[:, col:col + 128]
    flat, z = at_dev.flat, at_dev.z
    part = all_sum(part, flat, 8, [(d, (flat + i + 1) % 8) for i, d in enumerate(at_dev.plane)], nr, nb.at[0], 0, drain)
    part = all_sum(part, z, 4, [(d, (z + i + 1) % 4) for i, d in enumerate(at_dev.zothers)], nz, nb.at[1], 8)
    square_sum = jnp.sum(part, keepdims=True)
    clip = jnp.minimum(1.0, 1.0 / (jnp.sqrt(square_sum) + 1e-6))
    o_clip[...] = jnp.broadcast_to(clip, o_clip.shape)
    for i in range(7):
        sent(nb.at[0], norm_s.at[i])
    for i in range(3):
        sent(nb.at[1], norm_s.at[8 + i])


def gather_kernel(
    lr_ref, grad, clip_ref, master, mom1, mom2, o_master, o_mom1, o_mom2, o_work, gat_r, gcore_r, gcore_s, gp_s, gu_s, gd_s, gq_s,
):
    shard, width = grad.shape
    total_rows = o_work.shape[0]
    rows = shard // STREAMS
    tile = min(32, rows)
    at_dev = Place()
    me, c, m, chip = at_dev.me, at_dev.c, at_dev.m, at_dev.chip
    my_chip = me // 2

    barrier = pltpu.get_barrier_semaphore()
    for other in (at_dev.partner, at_dev.xn, at_dev.yn, at_dev.up):
        pl.semaphore_signal(barrier, inc=1, device_id=(other,), device_id_type=MESH)

    @pl.when(m == 1)
    def _():
        pl.semaphore_signal(barrier, inc=1, device_id=(at_dev.down,), device_id_type=MESH)

    learn_rate = lr_ref[0]
    inv1 = 1.0 / (1.0 - 0.9 ** ADAM_STEP)
    inv2 = 1.0 / (1.0 - 0.99 ** ADAM_STEP)
    decay_runs, fast_rows = rule_runs(width, total_rows)

    clip = jnp.broadcast_to(clip_ref[0:1, :], (tile, 128))

    def update(s):
        def rows_step(t):
            base = pl.multiple_of(t * tile, tile)
            out_at = pl.ds(pl.multiple_of(s * rows + t * tile, tile), tile)
            row = me * shard + s * rows + base + lax.broadcasted_iota(jnp.int32, (tile, 128), 0)
            decays = (row >= decay_runs[0][0]) & (row < decay_runs[0][1])
            for start, stop in decay_runs[1:]:
                decays = decays | ((row >= start) & (row < stop))
            fast = row == fast_rows[0]
            for fast_row in fast_rows[1:]:
                fast = fast | (row == fast_row)
            decay = jnp.where(decays, 0.1, 0.0)
            step_size = learn_rate * jnp.where(fast, 2.0, 1.0)
            for col in range(0, width, 128):
                cols = pl.ds(col, 128)
                g = grad[out_at, cols] * clip
                old = master[out_at, cols]
                first = 0.9 * mom1[out_at, cols] + 0.1 * g
                second = 0.99 * mom2[out_at, cols] + 0.01 * (g * g)
                new = old - step_size * ((first * inv1) / (jnp.sqrt(second * inv2) + 1e-8) + decay * old)
                o_master[out_at, cols] = new
                o_mom1[out_at, cols] = first
                o_mom2[out_at, cols] = second
                o_work[pl.ds(pl.multiple_of(me * shard + s * rows + base, tile), tile), cols] = new.astype(jnp.bfloat16)

        each(0, rows // tile, rows_step)

    update(0)
    pl.semaphore_wait(barrier, 4 + m)

    def work_rows(ci, s, cc):
        return o_work.at[pl.ds(pl.multiple_of((ci * 2 + cc) * shard + s * rows, rows), rows)]

    def send(src, ci, s, k, link):
        dst = work_rows(ci, s, c)
        i = ci * STREAMS + s
        if link == "c":
            remote(src, dst, gcore_s.at[i], gcore_r.at[i], at_dev.partner).start()
        else:
            to = {"p": at_dev.pn(s), "q": at_dev.qn(s), "u": at_dev.up, "d": at_dev.down}[link]
            ssem = {"p": gp_s, "q": gq_s, "u": gu_s, "d": gd_s}[link]
            remote(src, dst, ssem.at[s, k], gat_r.at[i], to).start()

    def gather_program(sends, own):
        first = [t for t in sends if t[:3] == own and t[4] == 0]

        def start_own(s):
            src = work_rows(my_chip, s, c)
            for u, qo, _, link, _ in first:
                send(src, my_chip, s, 2 * u + qo, link)

        start_own(0)

        def rest_own(s):
            update(s)
            start_own(s)

        each(1, STREAMS, rest_own)

        def settle(old):
            for (u, qo, _, link, group), n in old:
                def wait(s):
                    if link == "c":
                        ci = chip(s, u, qo, _)
                        ref = work_rows(ci, s, 1 - c)
                        i = ci * STREAMS + s
                        remote(ref, ref, gcore_s.at[i], gcore_r.at[i], me).wait()
                    else:
                        ssem = {"p": gp_s, "q": gq_s, "u": gu_s, "d": gd_s}[link]
                        remote(block_ref, block_ref, ssem.at[s, 2 * u + qo], gat_r.at[0], me).wait_send()

                each(group * GROUP, group * GROUP + GROUP, wait)

        block_ref = o_work.at[pl.ds(0, rows)]
        rest = [t for t in sends if t[:3] != own]
        pending = [(t, -1) for t in sends if t[:3] == own]
        seen = set()
        n = 0
        while n < len(rest):
            block, group = rest[n][:3], rest[n][4]
            links = [rest[n][3]]
            start = n
            while n + 1 < len(rest) and rest[n + 1][:3] == block and rest[n + 1][4] == group:
                n += 1
                links.append(rest[n][3])
            n += 1
            new = (block, group) not in seen
            seen.add((block, group))
            if new:
                settle([p for p in pending if p[1] <= start - LAG])
                pending = [p for p in pending if p[1] > start - LAG]

            def body(s, block=block, links=tuple(links), new=new):
                ci = chip(s, *block)
                ref = work_rows(ci, s, c)
                if new:
                    remote(ref, ref, gcore_s.at[0], gat_r.at[ci * STREAMS + s], me).wait_recv()
                for link in links:
                    send(ref, ci, s, 2 * block[0] + block[1], link)

            for s in range(group * GROUP, group * GROUP + GROUP):
                body(s)
            pending += [(t, start) for t in rest[start:n]]
        settle(pending)

    @pl.when(m == 0)
    def _():
        gather_program(END_SENDS, (0, 0, 0))

    @pl.when(m == 1)
    def _():
        gather_program(MID_SENDS, (1, 0, 0))


def store_kernel(*refs):
    ins, outs, sem = refs[:4], refs[4:8], refs[8]
    copies = [pltpu.make_async_copy(src, dst, sem.at[i]) for i, (src, dst) in enumerate(zip(ins[:3], outs[:3]))]
    pieces = sem.shape[0] - 3
    rows = ins[3].shape[0] // pieces
    for i in range(pieces):
        at = pl.ds(i * rows, rows)
        copies.append(pltpu.make_async_copy(ins[3].at[at], outs[3].at[at], sem.at[3 + i]))
    for copy in copies:
        copy.start()
    for copy in copies:
        copy.wait()


def solution(mesh):
    dev_count = mesh.shape["dp"]

    def device_step(local_grads, master, mom_first, mom_second, learn_rate):
        shard_rows, width = master.shape
        total_rows = shard_rows * dev_count
        rows = shard_rows // STREAMS
        any_spec = pl.BlockSpec(memory_space=pl.ANY)
        vmem_spec = pl.BlockSpec(memory_space=pltpu.VMEM)
        dma = pltpu.SemaphoreType.DMA
        f32, bf16 = jnp.float32, jnp.bfloat16
        shard = pltpu.VMEM((shard_rows, width), f32)
        grad_rows, clip, _ = pl.pallas_call(
            reduce_kernel,
            out_shape=[
                shard,
                pltpu.VMEM((8, 128), f32),
                jax.ShapeDtypeStruct((total_rows // 2, width), bf16),
            ],
            in_specs=[any_spec],
            out_specs=[vmem_spec] * 2 + [any_spec],
            scratch_shapes=[
                pltpu.VMEM((STREAMS, 8, rows, width), f32),
                pltpu.VMEM((STREAMS, 8, rows, width), f32),
                pltpu.VMEM((STREAMS, 5, rows, width), f32),
                pltpu.VMEM((STREAMS, 4, rows, width), f32),
                pltpu.VMEM((STREAMS, rows, width), f32),
                pltpu.VMEM((2, GROUP, 2, rows, width), bf16),
                pltpu.VMEM((8, width), f32),
                pltpu.VMEM((2, 8, 128), f32),
                pltpu.VMEM((8, 8, 128), f32),
                pltpu.VMEM((4, 8, 128), f32),
                dma((16 * STREAMS,)), dma((16 * STREAMS,)),
                dma((STREAMS, 8)), dma((STREAMS, 8)), dma((STREAMS,)),
                dma((STREAMS, 8)), dma((STREAMS, 5)), dma((STREAMS, 4)),
                dma((STREAMS, 2)), dma((STREAMS,)), dma((STREAMS,)),
                dma((2, GROUP, 2)),
                dma((12,)), dma((12,)),
            ],
            compiler_params=pltpu.CompilerParams(
                collective_id=0, has_side_effects=True, vmem_limit_bytes=217 * 2 ** 18
            ),
            name="reduce_rows",
        )(local_grads)
        new_master, new_first, new_second, working = pl.pallas_call(
            gather_kernel,
            out_shape=[shard, shard, shard, pltpu.VMEM((total_rows, width), bf16)],
            in_specs=[pl.BlockSpec(memory_space=pltpu.SMEM)] + [vmem_spec] * 5,
            out_specs=[vmem_spec] * 4,
            scratch_shapes=[
                dma((16 * STREAMS,)), dma((16 * STREAMS,)), dma((16 * STREAMS,)),
                dma((STREAMS, 8)), dma((STREAMS, 8)), dma((STREAMS, 8)), dma((STREAMS, 8)),
            ],
            compiler_params=pltpu.CompilerParams(
                collective_id=1, has_side_effects=True, vmem_limit_bytes=4 * 2 ** 20
            ),
            name="update_gather",
        )(learn_rate.reshape(1), grad_rows, clip, master, mom_first, mom_second)
        return pl.pallas_call(
            store_kernel,
            out_shape=[jax.ShapeDtypeStruct((shard_rows, width), f32)] * 3
            + [jax.ShapeDtypeStruct((total_rows, width), bf16)],
            in_specs=[vmem_spec] * 4,
            out_specs=[any_spec] * 4,
            scratch_shapes=[dma((3 + 8,))],
            compiler_params=pltpu.CompilerParams(vmem_limit_bytes=4 * 2 ** 20),
            name="store",
        )(new_master, new_first, new_second, working)

    return jax.shard_map(
        device_step,
        mesh=mesh,
        in_specs=(P("dp", None, None), P("dp", None), P("dp", None), P("dp", None), P()),
        out_specs=(P("dp", None), P("dp", None), P("dp", None), P(None, None)),
        check_vma=False,
    )
```
